512 devices in a mesh: tp: 16 (over z, core), ep: 32 (over y, x).
Axes of the slice: x: 4, y: 8, z: 8, core: 2. Of those that a mesh axis runs over, the one named last changes fastest.
Arguments:
- tokens: bfloat16 [12288, 2048], P('ep', 'tp'), may hold values from -6 to 6
- norm_gain: float32 [2048], replicated, may hold values from 0.25 to 1.75
- shared_gate: bfloat16 [2048, 2816], P('ep', 'tp'), may hold values from -0.125 to 0.125
- shared_up: bfloat16 [2048, 2816], P('ep', 'tp'), may hold values from -0.125 to 0.125
- shared_down: bfloat16 [2816, 2048], P('tp', 'ep'), may hold values from -0.21875 to 0.21875
- expert_gate: bfloat16 [16, 32, 176, 2048], P('tp', 'ep'), may hold values from -0.125 to 0.125
- expert_up: bfloat16 [16, 32, 176, 2048], P('tp', 'ep'), may hold values from -0.125 to 0.125
- expert_down: bfloat16 [64, 1408, 2048], P('ep', None, 'tp'), may hold values from -0.15625 to 0.15625
- chosen: int32 [64, 384], P('ep'), may hold values from 0 to 12287, as said below
- gates: float32 [64, 384], P('ep'), may hold values from 0.1 to 1
Outputs:
- mixed: bfloat16 [12288, 2048], P('ep', 'tp')
The draws below stay inside these ranges and needn't reach their ends.
Inputs may be any that keep to these rules, and one draw needn't show every extreme that they name: Each row of chosen holds 384 different token indices in rising order. Of one row, at most 24 lie among the 384 tokens of one index of ep (tokens s * 384 to (s + 1) * 384 - 1), and in every row exactly 24 lie among those of some index.
All inputs are finite; a program needn't handle non-finite values.
Results may differ from the reference program's by a relative error of at most 0.012.
Values may be sent and summed in bfloat16 or wider, within the bound.
A program may use at most 64 MiB of HBM per device.

```python
import jax
import jax.numpy as jnp
from jax import lax

D = 2048
FS = 2816
F = 1408
EXP_DEV = 2
TOK_DEV = 384
TOKENS = 12288
EXPERTS = 64
SPLIT = 8
CAP = 384
N_TP = 16
N_EP = 32


def expert_choices(expert_key):
    key_pair, key_shift, key_rank = jax.random.split(expert_key, 3)
    halves = N_EP // 2
    average = CAP // N_EP
    pairing = jax.random.permutation(key_pair, N_EP)
    shifts = jax.random.randint(key_shift, (halves,), 0, average + 1).astype(jnp.int32)
    shifts = shifts.at[0].set(average)
    counts = jnp.full((N_EP,), average, jnp.int32)
    counts = counts.at[pairing[:halves]].add(shifts).at[pairing[halves:]].add(-shifts)
    rank_keys = jax.random.split(key_rank, N_EP)
    rankings = jax.vmap(source_ranking)(rank_keys)
    flags = (rankings < counts[:, None]).reshape(-1).astype(jnp.int32)
    places = jnp.cumsum(flags) - 1
    places = jnp.where(flags > 0, places, CAP)
    token_ids = jnp.arange(N_EP * TOK_DEV, dtype=jnp.int32)
    return jnp.zeros((CAP,), jnp.int32).at[places].set(token_ids, mode='drop')


def source_ranking(rank_key):
    return jax.random.permutation(rank_key, TOK_DEV).astype(jnp.int32)


def draw_chosen(key, part):
    expert_keys = jax.random.split(jax.random.fold_in(key, 11), EXPERTS)
    return jax.vmap(expert_choices)(expert_keys)


def strengthened(array, own_key, source, target, shards_of, factor):
    owner, partner = [(jnp.arange(array.shape[position]) // (array.shape[position] // shards_of)).reshape([-1 if axis == position else 1 for axis in range(array.ndim)]) for position in (source, target)]
    chosen = jax.random.permutation(own_key, shards_of)[partner]
    strong = (owner == chosen) | (owner == (partner + shards_of // 2) % shards_of)
    return jnp.where(strong, factor * array, array)


def levels(stream_key, dims, cuts, low, top_value):
    def one(axis_at, shards_of):
        draws = jax.random.uniform(jax.random.fold_in(jax.random.fold_in(stream_key, 6), axis_at), (shards_of,), jnp.float32, low / len(cuts), top_value / len(cuts))
        return jnp.repeat(jnp.exp(draws), dims[axis_at] // shards_of).reshape((-1,) + (1,) * (len(dims) - axis_at - 1))

    level = one(*cuts[0])
    for cut in cuts[1:]:
        level = level * one(*cut)
    return level


def normal_values(key, shape, scale, most, cuts=(), held_as=jnp.bfloat16):
    entries = jax.random.normal(key, shape, jnp.float32) * scale
    if len(cuts) > 0:
        entries = levels(key, shape, cuts, -0.22, 0.18) * entries
    return jnp.clip(entries, min=-most, max=most).astype(held_as)


def bell_draw_with(own_key, extent, scale, reach, cuts, heavy, held_as=jnp.bfloat16):
    entries = scale * jax.random.normal(own_key, extent, jnp.float32)
    if cuts:
        entries = entries * levels(own_key, extent, cuts, -0.22, 0.18)
    return jnp.clip(strengthened(entries, jax.random.fold_in(own_key, 3), *heavy), -reach, reach).astype(held_as)


def setup_inputs(seed: int = 0) -> dict:
    key_list = jax.random.split(jax.random.key(seed), 11)
    tokens = normal_values(key_list[0], (TOKENS, D), 1.0, 6.0, ((0, 32), (1, 16)))
    norm_gain = jnp.clip(1.0 + 0.15 * jax.random.normal(key_list[1], (D,), jnp.float32), 0.25, 1.75)
    shared_gate = normal_values(key_list[2], (D, FS), D ** -0.5, 0.125, ((0, 32), (1, 16)))
    shared_up = normal_values(key_list[3], (D, FS), D ** -0.5, 0.125, ((0, 32), (1, 16)))
    shared_down = bell_draw_with(key_list[4], (FS, D), FS ** -0.5, 0.21875, ((0, 16), (1, 32)), (0, 1, 32, 2.75))
    expert_gate = normal_values(key_list[5], (N_TP, N_EP, F // SPLIT, D), D ** -0.5, 0.125, ((0, 16), (1, 32)))
    expert_up = normal_values(key_list[6], (N_TP, N_EP, F // SPLIT, D), D ** -0.5, 0.125, ((0, 16), (1, 32)))
    expert_down = normal_values(key_list[7], (EXPERTS, F, D), F ** -0.5, 0.15625, ((0, 32), (2, 16)))
    chosen = draw_chosen(jax.random.fold_in(key_list[10], 71), 0)
    gates = jnp.clip(0.1 + 0.9 * jax.random.uniform(key_list[9], (EXPERTS, CAP), jnp.float32) ** levels(key_list[9], (EXPERTS, CAP), ((0, 32),), -0.2, 0.2), 0.1, 1.0)
    return dict(tokens=tokens, norm_gain=norm_gain, shared_gate=shared_gate, shared_up=shared_up, shared_down=shared_down, expert_gate=expert_gate, expert_up=expert_up, expert_down=expert_down, chosen=chosen, gates=gates)


norm_eps = 1e-06

def reference(tokens, norm_gain, shared_gate, shared_up, shared_down, expert_gate, expert_up, expert_down, chosen, gates):
    widened = tokens.astype(jnp.float32)
    inv_scale = lax.rsqrt(lax.optimization_barrier(jnp.mean(widened * widened, axis=1, keepdims=True)) + norm_eps)
    normed = (widened * inv_scale * norm_gain.astype(jnp.float32)).astype(jnp.bfloat16)
    gate_sum = jnp.dot(normed, shared_gate, preferred_element_type=jnp.float32)
    up_sum = jnp.dot(normed, shared_up, preferred_element_type=jnp.float32)
    shared_hidden = (jax.nn.silu(gate_sum) * up_sum).astype(jnp.bfloat16)
    shared_out = jnp.dot(shared_hidden, shared_down, preferred_element_type=jnp.float32)
    split_count = N_TP // EXP_DEV

    def expert_term(expert_index):
        ep_column = (expert_index // EXP_DEV).astype(jnp.int32)
        expert_slot = (expert_index % EXP_DEV).astype(jnp.int32)

        def weight_of(weights):
            picked = lax.dynamic_index_in_dim(weights, ep_column, 1, keepdims=False)
            picked = lax.dynamic_slice_in_dim(picked, expert_slot * split_count, split_count, 0)
            return jnp.transpose(picked.reshape(F, D))
        token_ids = lax.dynamic_index_in_dim(chosen, expert_index, 0, keepdims=False)
        token_rows = jnp.take(normed, token_ids, axis=0)
        gate_values = jnp.dot(token_rows, weight_of(expert_gate), preferred_element_type=jnp.float32)
        up_values = jnp.dot(token_rows, weight_of(expert_up), preferred_element_type=jnp.float32)
        hidden = (jax.nn.silu(gate_values) * up_values).astype(jnp.bfloat16)
        down_weight = lax.dynamic_index_in_dim(expert_down, expert_index, 0, keepdims=False)
        outputs = jnp.dot(hidden, down_weight, preferred_element_type=jnp.float32)
        gate_row = lax.dynamic_index_in_dim(gates, expert_index, 0, keepdims=False).astype(jnp.float32)
        return (gate_row[:, None] * outputs).astype(jnp.bfloat16)
    weighted = lax.map(expert_term, jnp.arange(EXPERTS, dtype=jnp.int32))
    routed = jnp.zeros((TOKENS, D), jnp.float32).at[chosen.reshape(-1)].add(weighted.reshape(-1, D).astype(jnp.float32))
    return (shared_out + routed).astype(jnp.bfloat16)
```

```python
import functools

import jax
import jax.numpy as jnp
from jax import lax
from jax.experimental import pallas as pl
from jax.experimental.pallas import tpu as pltpu
from jax.sharding import PartitionSpec as P

MESH = pl.DeviceIdType.MESH
EXP_DEV = 2
TOK_DEV = 384
CAP = 384
NZ, NY, NX = 8, 8, 4
N_TP, N_EP = 16, 32
SLOT = 24
PER = EXP_DEV * SLOT
SLOTS = N_EP * PER
F_DEV = 176
D = 2048
W = 128
norm_eps = 1e-06
bf16 = jnp.bfloat16
f32 = jnp.float32


class Link:
    def __init__(self, send_sems, recv_sems):
        self.send_sems, self.recv_sems = send_sems, recv_sems
        self.keys, self.sent = {}, []

    def _at(self, key):
        return self.keys.setdefault(key, len(self.keys))

    def _copy(self, src, dst, key, device):
        i = self._at(key)
        return pltpu.make_async_remote_copy(
            src_ref=src,
            dst_ref=dst,
            send_sem=self.send_sems.at[i],
            recv_sem=self.recv_sems.at[i],
            device_id=device,
            device_id_type=MESH,
        )

    def send(self, src, dst, key, device):
        copy = self._copy(src, dst, key, device)
        copy.start()
        self.sent.append(copy)

    def arrive(self, dst, key, device):
        self._copy(dst, dst, key, device).wait_recv()

    def finish(self):
        for copy in self.sent:
            copy.wait_send()


def places():
    tp, ep = lax.axis_index("tp"), lax.axis_index("ep")
    return tp // 2, lax.rem(tp, 2), ep // NX, lax.rem(ep, NX)


def around(position, step, count):
    return lax.rem(position + step + count, count)


def z_device(z, core):
    return {"tp": z * 2 + core}


def greet(z_ring, plane, lines):
    barrier = pltpu.get_barrier_semaphore()
    z, core, y, x = places()
    devices = []
    if z_ring:
        devices += [z_device(around(z, 1, NZ), core), z_device(around(z, -1, NZ), core)]
        devices += [z_device(z, 1 - core)]
    if plane:
        devices += [{"ep": around(y, a, NY) * NX + around(x, b, NX)} for a, b in OFFSETS]
    if lines:
        devices += [{"ep": around(y, a, NY) * NX + x} for a in (1, -1)]
        devices += [{"ep": y * NX + around(x, b, NX)} for b in (1, -1)]
    for device in devices:
        pl.semaphore_signal(barrier, inc=1, device_id=device, device_id_type=MESH)
    return len(devices)


def met(count):
    pl.semaphore_wait(pltpu.get_barrier_semaphore(), count)


OFFSETS = sorted(
    [(a, b) for a in range(-3, 5) for b in range(-1, 3) if (a, b) != (0, 0)],
    key=lambda o: (-abs(o[0]) - abs(o[1]), o),
)


def exchange_start(src, dst, send_sem, recv_sem):
    _, _, y, x = places()
    own = y * NX + x
    for a, b in OFFSETS:
        peer = around(y, a, NY) * NX + around(x, b, NX)
        pltpu.make_async_remote_copy(
            src_ref=src.at[peer],
            dst_ref=dst.at[own],
            send_sem=send_sem,
            recv_sem=recv_sem,
            device_id={"ep": peer},
            device_id_type=MESH,
        ).start()
    dst[own] = src[own]


def exchange_wait(src, dst, send_sem, recv_sem):
    part = pl.ds(0, N_EP - 1)
    pltpu.make_async_copy(dst.at[part], dst.at[part], recv_sem).wait()
    pltpu.make_async_copy(src.at[part], src.at[part], send_sem).wait()


def reach(direction, flipped):
    return 4 if (direction > 0) != bool(flipped) else 3


def ring_gather(src, dst, link, cuts):
    z, core, _, _ = places()
    own = z * 2 + core
    other = z_device(z, 1 - core)
    beside = {d: z_device(around(z, d, NZ), core) for d in (1, -1)}
    for h, rows in enumerate(cuts):
        for d in (1, -1):
            link.send(src.at[rows], dst.at[own, rows], (d, 1, h), beside[d])
    for h, rows in enumerate(cuts):
        link.send(src.at[rows], dst.at[own, rows], ("core", 0, 0, h), other)
    dst[own] = src[...]
    yield
    for k in range(1, 5):
        for h, rows in enumerate(cuts):
            for d in (1, -1):
                most = reach(d, h % 2)
                if k > most:
                    continue
                block = dst.at[around(z, -d * k, NZ) * 2 + core, rows]
                link.arrive(block, (d, k, h), other)
                if k < most:
                    link.send(block, block, (d, k + 1, h), beside[d])
                link.send(block, block, ("core", d, k, h), other)
                yield
    for h, rows in enumerate(cuts):
        link.arrive(dst.at[z * 2 + 1 - core, rows], ("core", 0, 0, h), other)
    for k in range(1, 5):
        for h, rows in enumerate(cuts):
            for d in (1, -1):
                if k <= reach(d, h % 2):
                    block = dst.at[around(z, -d * k, NZ) * 2 + 1 - core, rows]
                    link.arrive(block, ("core", d, k, h), other)
                    yield
    link.finish()


def plane_gather(src, dst, link, y_first):
    _, _, y, x = places()
    a, na, b, nb = (y, NY, x, NX) if y_first else (x, NX, y, NY)

    def index(p, q):
        return p * NX + q if y_first else q * NX + p

    own = index(a, b)
    here = {"ep": own}
    along = {d: {"ep": index(around(a, d, na), b)} for d in (1, -1)}
    across = {d: {"ep": index(a, around(b, d, nb))} for d in (1, -1)}
    for d in (1, -1):
        link.send(src, dst.at[own], ("a", d, 1), along[d])
    for d in (1, -1):
        link.send(src, dst.at[own], ("b", d, 1, 0, 0), across[d])
    dst[own] = src[...]
    yield
    tags = [(0, 0)]
    for k in range(1, na // 2 + 1):
        for d in (1, -1):
            most = na // 2 if d > 0 else na // 2 - 1
            if k > most:
                continue
            tags.append((d, k))
            block = dst.at[index(around(a, -d * k, na), b)]
            link.arrive(block, ("a", d, k), here)
            if k < most:
                link.send(block, block, ("a", d, k + 1), along[d])
            for s in (1, -1):
                link.send(block, block, ("b", s, 1, d, k), across[s])
            yield
    for j in range(1, nb // 2 + 1):
        for n, (d, k) in enumerate(tags):
            for s in (1, -1):
                most = nb // 2 if (s > 0) == (n % 2 == 0) else nb // 2 - 1
                if j > most:
                    continue
                block = dst.at[index(around(a, -d * k, na), around(b, -s * j, nb))]
                link.arrive(block, ("b", s, j, d, k), here)
                if j < most:
                    link.send(block, block, ("b", s, j + 1, d, k), across[s])
                yield
    link.finish()


def in_turn(*jobs):
    jobs = list(jobs)
    while jobs:
        for job in list(jobs):
            try:
                next(job)
            except StopIteration:
                jobs.remove(job)


def one_hot(condition):
    return jnp.where(condition, 1.0, 0.0).astype(bf16)


def ask_kernel(req_ref, asked_ref, send_sem, recv_sem):
    met(greet(False, True, False))
    exchange_start(req_ref, asked_ref, send_sem, recv_sem)
    exchange_wait(req_ref, asked_ref, send_sem, recv_sem)


def dispatch_kernel(ids_ref, tok_ref, came_ref, all_ref, out, send_sem, recv_sem, ss, rs):
    count = greet(True, True, False)
    token = lax.broadcasted_iota(jnp.int32, (SLOTS, TOK_DEV), 1)
    picked = jnp.dot(one_hot(token == ids_ref[...]), tok_ref[...], preferred_element_type=f32)
    out[...] = picked.astype(bf16).reshape(N_EP, PER, W)
    met(count)
    exchange_start(out, came_ref, send_sem, recv_sem)
    half = TOK_DEV // 2
    in_turn(ring_gather(tok_ref, all_ref, Link(ss, rs), [pl.ds(0, half), pl.ds(half, half)]))
    exchange_wait(out, came_ref, send_sem, recv_sem)


def join_kernel(slot_ref, came_ref, gu_ref, dn_ref, rows_ref, wg_ref, wd_ref, own, ss, rs, sg, rg, sd, rd):
    count = greet(True, False, True)
    slot = lax.broadcasted_iota(jnp.int32, (EXP_DEV * CAP, SLOTS), 1)
    came = came_ref[...].reshape(SLOTS, W)
    own[...] = jnp.dot(
        one_hot(slot == slot_ref[...]), came, preferred_element_type=f32
    ).astype(bf16)
    met(count)
    in_turn(
        ring_gather(own, rows_ref, Link(ss, rs), [pl.ds(0, CAP), pl.ds(CAP, CAP)]),
        plane_gather(gu_ref, wg_ref, Link(sg, rg), True),
        plane_gather(dn_ref, wd_ref, Link(sd, rd), False),
    )


def hidden_kernel(own_ref, all_ref, ss, rs):
    met(greet(True, False, False))
    in_turn(ring_gather(own_ref, all_ref, Link(ss, rs), [pl.ds(0, 96), pl.ds(96, 80)]))


def back_kernel(
    slot_ref, ids_ref, rows_ref, part_ref, mixed_ref, out, came, pair, got, made, send_sem, recv_sem, ss, rs
):
    count = greet(True, True, False)
    z, core, _, _ = places()
    other = z_device(z, 1 - core)
    slot = lax.broadcasted_iota(jnp.int32, (SLOTS, EXP_DEV * CAP), 0)
    spread = jnp.dot(one_hot(slot == slot_ref[...]), rows_ref[...], preferred_element_type=f32)
    out[...] = spread.astype(bf16).reshape(N_EP, PER, W)
    met(count)
    link = Link(ss, rs)
    order = [4, -4 + 1, 3, -2, 2, -1, 1, 0]
    targets = {m % NZ: around(z, m, NZ) for m in order}
    for m in order:
        at = targets[m % NZ]
        link.send(part_ref.at[at * 2 + 1 - core], pair.at[at], ("core", m % NZ), other)
    exchange_start(out, came, send_sem, recv_sem)
    half = TOK_DEV // 2
    here = set()

    def term(m, rows):
        m = m % NZ
        at = targets[m]
        if m not in here:
            link.arrive(pair.at[at], ("core", m), other)
            here.add(m)
        return part_ref[at * 2 + core, rows].astype(f32) + pair[at, rows].astype(f32)

    cuts = [pl.ds(0, half), pl.ds(half, half)]
    way = {1: 0, -1: 1}
    for k in range(1, 5):
        for h, rows in enumerate(cuts):
            for d in (1, -1):
                most = reach(d, h)
                if k > most:
                    continue
                total = term(d * (most + 1 - k), rows)
                if k > 1:
                    link.arrive(got.at[way[d], k - 1, rows], (d, k - 1, h), other)
                    total = total + got[way[d], k - 1, rows].astype(f32)
                made[way[d], k, rows] = total.astype(bf16)
                link.send(
                    made.at[way[d], k, rows],
                    got.at[way[d], k, rows],
                    (d, k, h),
                    z_device(around(z, d, NZ), core),
                )
    exchange_wait(out, came, send_sem, recv_sem)
    token = lax.broadcasted_iota(jnp.int32, (TOK_DEV, SLOTS), 0)
    routed = jnp.dot(
        one_hot(token == ids_ref[...]), came[...].reshape(SLOTS, W), preferred_element_type=f32
    )
    for h, rows in enumerate(cuts):
        total = term(0, rows)
        for d in (1, -1):
            most = reach(d, h)
            link.arrive(got.at[way[d], most, rows], (d, most, h), other)
            total = total + got[way[d], most, rows].astype(f32)
        mixed_ref[rows, :] = (total + routed[h * half : (h + 1) * half]).astype(bf16)
    link.finish()


def call(kernel, name, ident, operands, outs, scratch):
    vmem = pl.BlockSpec(memory_space=pltpu.VMEM)
    return pl.pallas_call(
        kernel,
        name=name,
        out_shape=[jax.ShapeDtypeStruct(s, d) for s, d in outs],
        in_specs=[vmem] * len(operands),
        out_specs=[vmem] * len(outs),
        scratch_shapes=scratch,
        compiler_params=pltpu.CompilerParams(
            collective_id=ident, has_side_effects=True, vmem_limit_bytes=48 * 1024 * 1024
        ),
    )(*operands)


def sems(n):
    return [pltpu.SemaphoreType.DMA((n,)), pltpu.SemaphoreType.DMA((n,))]


def pair_sems():
    return [pltpu.SemaphoreType.DMA, pltpu.SemaphoreType.DMA]


def scaled(rows, gain):
    wide = jnp.moveaxis(rows, 0, 1).reshape(rows.shape[1], D).astype(f32)
    inv = lax.rsqrt(jnp.mean(wide * wide, axis=1, keepdims=True) + norm_eps)
    return (wide * inv * gain).astype(bf16)


def on_device(
    tokens,
    norm_gain,
    shared_gate,
    shared_up,
    shared_down,
    expert_gate,
    expert_up,
    expert_down,
    chosen,
    gates,
):
    sources = chosen // TOK_DEV
    before = jnp.sum((sources[:, None, :] < sources[:, :, None]).astype(jnp.int32), axis=2)
    rank = jnp.arange(CAP, dtype=jnp.int32)[None, :] - before
    base = jnp.arange(EXP_DEV, dtype=jnp.int32)[:, None] * SLOT
    slots = sources * PER + base + rank
    local_ids = chosen - sources * TOK_DEV
    place = (
        jnp.arange(N_EP, dtype=jnp.int32)[None, :, None] * PER
        + base[:, :, None]
        + jnp.arange(SLOT, dtype=jnp.int32)[None, None, :]
    )
    requests = jnp.max(
        jnp.where(place[:, :, :, None] == slots[:, None, None, :], local_ids[:, None, None, :], -1),
        axis=3,
    )
    requests = jnp.moveaxis(requests, 0, 1).reshape(N_EP, 1, PER)
    requests = jnp.pad(requests, ((0, 0), (0, 0), (0, W - PER)), constant_values=-1)
    (asked,) = call(
        ask_kernel, "ask", 0, [requests], [((N_EP, 1, W), jnp.int32)], pair_sems()
    )
    asked = asked[:, 0, :PER].reshape(SLOTS)

    came, all_tokens = call(
        dispatch_kernel,
        "dispatch",
        1,
        [asked.reshape(SLOTS, 1), tokens],
        [((N_EP, PER, W), bf16), ((N_TP, TOK_DEV, W), bf16)],
        [pltpu.VMEM((N_EP, PER, W), bf16), *pair_sems(), *sems(32)],
    )

    edge = lambda a: a[:, W:]
    gu = jnp.concatenate(
        [
            shared_gate[:, :W],
            shared_up[:, :W],
            edge(shared_gate),
            edge(shared_up),
            jnp.zeros((64, 32), bf16),
        ],
        axis=1,
    )
    dn = jnp.pad(shared_down.T, ((0, 0), (0, 80)))
    rows, wg, wd = call(
        join_kernel,
        "join",
        2,
        [slots.reshape(EXP_DEV * CAP, 1), came, gu, dn],
        [((N_TP, EXP_DEV * CAP, W), bf16), ((N_EP, 64, 384), bf16), ((N_EP, 64, 256), bf16)],
        [pltpu.VMEM((EXP_DEV * CAP, W), bf16), *sems(32), *sems(32), *sems(32)],
    )

    expert = lax.axis_index("tp") // (N_TP // EXP_DEV)
    own_rows = lax.dynamic_slice_in_dim(rows, expert * CAP, CAP, axis=1)
    token_rows = scaled(own_rows, norm_gain)
    gate_weight = expert_gate.reshape(F_DEV, D)
    up_weight = expert_up.reshape(F_DEV, D)
    gate_values = jnp.einsum("hd,rd->hr", gate_weight, token_rows, preferred_element_type=f32)
    up_values = jnp.einsum("hd,rd->hr", up_weight, token_rows, preferred_element_type=f32)
    part_hidden = (jax.nn.silu(gate_values) * up_values).astype(bf16)

    (all_hidden,) = call(
        hidden_kernel, "hidden", 3, [part_hidden], [((N_TP, F_DEV, CAP), bf16)], sems(32)
    )
    all_hidden = all_hidden.reshape(EXP_DEV, N_TP // EXP_DEV * F_DEV, CAP)
    outputs = jnp.einsum("efr,efd->erd", all_hidden, expert_down, preferred_element_type=f32)
    weighted = (gates[:, :, None] * outputs).astype(bf16).reshape(EXP_DEV * CAP, W)

    normed = scaled(all_tokens, norm_gain)
    sums = jnp.dot(normed, wg.reshape(D, 384), preferred_element_type=f32)
    low = jax.nn.silu(sums[:, :W]) * sums[:, W : 2 * W]
    high = jax.nn.silu(sums[:, 256:304]) * sums[:, 304:352]
    shared_hidden = jnp.concatenate([low, high, jnp.zeros((TOK_DEV, 80), f32)], axis=1).astype(bf16)
    blocks = jnp.einsum(
        "rh,tdh->trd", shared_hidden, wd.reshape(N_TP, W, 256), preferred_element_type=f32
    ).astype(bf16)

    (mixed,) = call(
        back_kernel,
        "back",
        4,
        [slots.reshape(1, EXP_DEV * CAP), asked.reshape(1, SLOTS), weighted, blocks],
        [((TOK_DEV, W), bf16)],
        [
            pltpu.VMEM((N_EP, PER, W), bf16),
            pltpu.VMEM((N_EP, PER, W), bf16),
            pltpu.VMEM((NZ, TOK_DEV, W), bf16),
            pltpu.VMEM((2, 5, TOK_DEV, W), bf16),
            pltpu.VMEM((2, 5, TOK_DEV, W), bf16),
            *pair_sems(),
            *sems(32),
        ],
    )
    return mixed


def solution(mesh):
    return jax.shard_map(
        on_device,
        mesh=mesh,
        in_specs=(
            P("ep", "tp"),
            P(),
            P("ep", "tp"),
            P("ep", "tp"),
            P("tp", "ep"),
            P("tp", "ep", None, None),
            P("tp", "ep", None, None),
            P("ep", None, "tp"),
            P("ep", None),
            P("ep", None),
        ),
        out_specs=P("ep", "tp"),
        check_vma=False,
    )
```

```python
import jax
import jax.numpy as jnp
from jax import lax
from jax.experimental import pallas as pl
from jax.experimental.pallas import tpu as pltpu
from jax.sharding import PartitionSpec as P

MESH = pl.DeviceIdType.MESH
EXP_DEV = 2
TOK_DEV = 384
CAP = 384
NZ, NY, NX = 8, 8, 4
N_TP, N_EP = 16, 32
SLOT, ROOM = 24, 32
F_DEV, F = 176, 1408
D, W = 2048, 128
norm_eps = 1e-06
bf16, f32, i32 = jnp.bfloat16, jnp.float32, jnp.int32


class Link:
    def __init__(self, send_sems, recv_sems):
        self.send_sems, self.recv_sems = send_sems, recv_sems
        self.keys, self.sent = {}, []

    def _copy(self, src, dst, key, device):
        i = self.keys.setdefault(key, len(self.keys))
        return pltpu.make_async_remote_copy(
            src_ref=src,
            dst_ref=dst,
            send_sem=self.send_sems.at[i],
            recv_sem=self.recv_sems.at[i],
            device_id=device,
            device_id_type=MESH,
        )

    def send(self, src, dst, key, device):
        copy = self._copy(src, dst, key, device)
        copy.start()
        self.sent.append(copy)

    def arrive(self, dst, key, device):
        self._copy(dst, dst, key, device).wait_recv()

    def finish(self):
        for copy in self.sent:
            copy.wait_send()


def places():
    tp, ep = lax.axis_index("tp"), lax.axis_index("ep")
    return tp // 2, lax.rem(tp, 2), ep // NX, lax.rem(ep, NX)


def around(position, step, count):
    return lax.rem(position + step + count, count)


def z_device(z, core):
    return {"tp": z * 2 + core}


OFFSETS = sorted(
    [(a, b) for a in range(-3, 5) for b in range(-1, 3) if (a, b) != (0, 0)],
    key=lambda o: (o[1] % 4, o[0] % 8),
)


def greet():
    barrier = pltpu.get_barrier_semaphore()
    z, core, y, x = places()
    devices = [{"ep": around(y, a, NY) * NX + around(x, b, NX)} for a, b in OFFSETS]
    devices += [z_device(around(z, 1, NZ), core), z_device(around(z, -1, NZ), core)]
    devices += [z_device(z, 1 - core)]
    for device in devices:
        pl.semaphore_signal(barrier, inc=1, device_id=device, device_id_type=MESH)
    return len(devices)


class Exchange:
    def __init__(self, src, dst, src_all, dst_all, sems):
        self.src, self.dst, self.src_all, self.dst_all, self.sems = src, dst, src_all, dst_all, sems

    def start(self):
        _, _, y, x = places()
        own = y * NX + x
        for a, b in OFFSETS:
            peer = around(y, a, NY) * NX + around(x, b, NX)
            pltpu.make_async_remote_copy(
                src_ref=self.src(peer),
                dst_ref=self.dst(own),
                send_sem=self.sems.at[0],
                recv_sem=self.sems.at[1],
                device_id={"ep": peer},
                device_id_type=MESH,
            ).start()
        self.dst(own)[...] = self.src(own)[...]

    def arrive(self):
        part = self.dst_all
        pltpu.make_async_copy(part, part, self.sems.at[1]).wait()

    def finish(self):
        part = self.src_all
        pltpu.make_async_copy(part, part, self.sems.at[0]).wait()


def reach(direction, flipped):
    return 4 if (direction > 0) != bool(flipped) else 3


def ring_gather(pieces, link):
    z, core, _, _ = places()
    own = z * 2 + core
    other = z_device(z, 1 - core)
    beside = {d: z_device(around(z, d, NZ), core) for d in (1, -1)}
    for h, (flip, src, at) in enumerate(pieces):
        for d in (1, -1):
            link.send(src, at(own), (d, 1, h), beside[d])
    for h, (flip, src, at) in enumerate(pieces):
        link.send(src, at(own), ("core", 0, 0, h), other)
    for flip, src, at in pieces:
        at(own)[...] = src[...]
    yield
    for k in range(1, 5):
        for h, (flip, src, at) in enumerate(pieces):
            for d in (1, -1):
                most = reach(d, flip)
                if k > most:
                    continue
                block = at(around(z, -d * k, NZ) * 2 + core)
                link.arrive(block, (d, k, h), other)
                if k < most:
                    link.send(block, block, (d, k + 1, h), beside[d])
                link.send(block, block, ("core", d, k, h), other)
        yield
    for h, (flip, src, at) in enumerate(pieces):
        link.arrive(at(own + 1 - 2 * core), ("core", 0, 0, h), other)
        for k in range(1, 5):
            for d in (1, -1):
                if k <= reach(d, flip):
                    block = at(around(z, -d * k, NZ) * 2 + 1 - core)
                    link.arrive(block, ("core", d, k, h), other)
    yield


def plane_gather(src, dst, link, y_first):
    _, _, y, x = places()
    a, na, b, nb = (y, NY, x, NX) if y_first else (x, NX, y, NY)

    def index(p, q):
        return p * NX + q if y_first else q * NX + p

    own = index(a, b)
    here = {"ep": own}
    along = {d: {"ep": index(around(a, d, na), b)} for d in (1, -1)}
    across = {d: {"ep": index(a, around(b, d, nb))} for d in (1, -1)}
    for d in (1, -1):
        link.send(src, dst.at[own], ("a", d, 1), along[d])
    dst[own] = src[...]
    yield
    tags = [(0, 0)]
    for k in range(1, na // 2 + 1):
        for d in (1, -1):
            most = na // 2 if d > 0 else na // 2 - 1
            if k > most:
                continue
            tags.append((d, k))
            block = dst.at[index(around(a, -d * k, na), b)]
            link.arrive(block, ("a", d, k), here)
            if k < most:
                link.send(block, block, ("a", d, k + 1), along[d])
            yield
    for n, (d, k) in enumerate(tags):
        block = dst.at[index(around(a, -d * k, na), b)]
        for s in (1, -1):
            link.send(src if n == 0 else block, block, ("b", s, 1, n), across[s])
    yield
    for j in range(1, nb // 2 + 1):
        for n, (d, k) in enumerate(tags):
            for s in (1, -1):
                most = nb // 2 if (s > 0) == (n % 2 == 0) else nb // 2 - 1
                if j > most:
                    continue
                block = dst.at[index(around(a, -d * k, na), around(b, -s * j, nb))]
                link.arrive(block, ("b", s, j, n), here)
                if j < most:
                    link.send(block, block, ("b", s, j + 1, n), across[s])
                yield


def go(job, steps=1000):
    for _ in range(steps):
        if next(job, "end") == "end":
            return


def one_hot(condition):
    return jnp.where(condition, 1.0, 0.0).astype(bf16)


def silu(v):
    return v / (1.0 + jnp.exp(-v))


def dims(a, b):
    return (((a,), (b,)), ((), ()))


def normalise(blocks, gain_ref, out_ref):
    for r in range(0, TOK_DEV, W):
        rows = pl.ds(r, W)
        squares = jnp.zeros((W, W), f32)
        for t in range(N_TP):
            wide = blocks(t)[rows, :].astype(f32)
            squares = squares + wide * wide
        inv = lax.rsqrt(jnp.sum(squares, axis=1, keepdims=True) * (1.0 / D) + norm_eps)
        for t in range(N_TP):
            lanes = slice(t * W, (t + 1) * W)
            wide = blocks(t)[rows, :].astype(f32)
            out_ref[rows, lanes] = (wide * inv * gain_ref[:, lanes]).astype(bf16)


def layer_kernel(
    req_ref, col_ref, row_ref, tok_ref, gain_ref, gu_ref, dn_ref, gates_ref, eg_hbm, eu_hbm, ed_hbm,
    mixed_ref,
    asked, one_t, join, spread, out, came, tok_all, own, rows_all, wg, wd, hid, hid_all, back, returned,
    part, pair, got, made, eg, eu, ed, ed_t, normed, taken,
    load_sem, ask_sem, go_a, go_b, back_a, back_b,
    tok_s, tok_r, xa_s, xa_r, xb_s, xb_r, gu_s, gu_r, dn_s, dn_r, hid_s, hid_r, sum_s, sum_r,
):
    count = greet()
    z, core, _, _ = places()
    other = z_device(z, 1 - core)
    loads = [
        pltpu.make_async_copy(s, d, load_sem.at[i])
        for i, (s, d) in enumerate(((eg_hbm, eg), (eu_hbm, eu), (ed_hbm, ed)))
    ]
    for load in loads:
        load.start()
    came[...] = jnp.zeros_like(came)
    returned[...] = jnp.zeros_like(returned)
    for e in range(EXP_DEV):
        at = lax.broadcasted_iota(i32, (CAP, N_EP * ROOM), 1)
        join[e] = one_hot(at == col_ref[e])
    pl.semaphore_wait(pltpu.get_barrier_semaphore(), count)

    half = TOK_DEV // 2
    cuts = [pl.ds(0, half), pl.ds(half, half)]
    first = pl.ds(0, SLOT)
    some = pl.ds(0, N_EP - 1)

    ask = Exchange(
        lambda p: req_ref.at[p], lambda p: asked.at[p], req_ref.at[some], asked.at[some], ask_sem
    )
    ask.start()
    tok_link = Link(tok_s, tok_r)
    tok_ring = ring_gather(
        [(h, tok_ref.at[c], lambda t, c=c: tok_all.at[t, c]) for h, c in enumerate(cuts)], tok_link
    )
    go(tok_ring, 1)
    gu_link, dn_link = Link(gu_s, gu_r), Link(dn_s, dn_r)
    gu_job = plane_gather(gu_ref, wg, gu_link, True)
    dn_job = plane_gather(dn_ref, wd, dn_link, False)
    go(gu_job, 1)
    go(dn_job, 1)
    for e in range(EXP_DEV):
        at = lax.broadcasted_iota(i32, (N_EP * ROOM, CAP), 0)
        spread[e] = one_hot(at == row_ref[e])
    go(tok_ring, 1)
    go(gu_job, 2)
    go(dn_job, 2)

    ask.arrive()
    token = lax.broadcasted_iota(i32, (TOK_DEV, W), 0)
    for i in range(N_EP // 2):
        ids = jnp.maximum(asked[2 * i], asked[2 * i + 1])
        one_t[:, i * W : (i + 1) * W] = one_hot(token == ids)
    for i in range(4):
        lanes = slice(i * 512, (i + 1) * 512)
        picked = lax.dot_general(
            one_t[:, lanes], tok_ref[...], dims(0, 0), preferred_element_type=f32
        )
        out[i * 8 : (i + 1) * 8] = picked.astype(bf16).reshape(8, EXP_DEV, ROOM, W)
    dispatch = [
        Exchange(
            lambda p, e=e: out.at[p, e, first],
            lambda p, e=e: came.at[e, p, first],
            out.at[some, e, first],
            came.at[e, some, first],
            sem,
        )
        for e, sem in enumerate((go_a, go_b))
    ]
    for e in range(EXP_DEV):
        dispatch[e].start()
    go(tok_ring, 1)
    go(gu_job, 2)
    go(dn_job, 1)
    for load in loads:
        load.wait()
    for e in range(EXP_DEV):
        ed_t[e] = ed[e].T
    go(tok_ring, 1)
    go(gu_job, 2)

    x_links = [Link(xa_s, xa_r), Link(xb_s, xb_r)]
    x_rings = []
    for e in range(EXP_DEV):
        dispatch[e].arrive()
        own[e] = jnp.dot(
            join[e], came[e].reshape(N_EP * ROOM, W), preferred_element_type=f32
        ).astype(bf16)
        x_rings.append(
            ring_gather(
                [
                    (e + h, own.at[e, c], lambda t, c=c, e=e: rows_all.at[t, e, c])
                    for h, c in enumerate(cuts)
                ],
                x_links[e],
            )
        )
        go(x_rings[e], 1)
    go(tok_ring)
    go(gu_job, 2)
    go(dn_job, 1)
    for k in range(4):
        for e in range(EXP_DEV):
            go(x_rings[e], 1)
        if k > 0:
            go(gu_job, 6)
            go(dn_job, 6)
    for e in range(EXP_DEV):
        go(x_rings[e], 1)

    expert = z // (NZ // EXP_DEV)
    normalise(lambda t: rows_all.at[t, expert], gain_ref, taken)
    gate_values = lax.dot_general(eg[...], taken[...], dims(1, 1), preferred_element_type=f32)
    up_values = lax.dot_general(eu[...], taken[...], dims(1, 1), preferred_element_type=f32)
    hid[...] = (silu(gate_values) * up_values).astype(bf16)
    hid_link = Link(hid_s, hid_r)
    hid_ring = ring_gather(
        [
            (h, hid.at[c], lambda t, c=c: hid_all.at[t, c])
            for h, c in enumerate((pl.ds(0, 96), pl.ds(96, 80)))
        ],
        hid_link,
    )
    go(hid_ring, 1)

    normalise(lambda t: tok_all.at[t], gain_ref, normed)
    go(hid_ring, 1)
    go(gu_job)
    sums = jnp.dot(normed[...], wg[...].reshape(D, 384), preferred_element_type=f32)
    low = silu(sums[:, :W]) * sums[:, W : 2 * W]
    high = silu(sums[:, 256:304]) * sums[:, 304:352]
    shared = jnp.concatenate([low, high, jnp.zeros((TOK_DEV, 80), f32)], axis=1).astype(bf16)
    go(hid_ring, 1)
    go(dn_job)
    for t in range(N_TP):
        block = lax.dot_general(
            shared, wd[2 * t : 2 * t + 2].reshape(W, 256), dims(1, 1), preferred_element_type=f32
        )
        part[t] = block.astype(bf16)
    go(hid_ring, 1)

    link = Link(sum_s, sum_r)
    order = [4, -3, 3, -2, 2, -1, 1, 0]
    targets = {m % NZ: around(z, m, NZ) for m in order}
    for m in order:
        at = targets[m % NZ]
        link.send(part.at[at * 2 + 1 - core], pair.at[at], ("core", m % NZ), other)
    here = set()

    def term(m, rows):
        m = m % NZ
        at = targets[m]
        if m not in here:
            link.arrive(pair.at[at], ("core", m), other)
            here.add(m)
        return part[at * 2 + core, rows].astype(f32) + pair[at, rows].astype(f32)

    go(hid_ring)

    give = []
    for e in range(EXP_DEV):
        full = hid_all[e * 8 : (e + 1) * 8].reshape(F, CAP)
        outputs = jnp.dot(ed_t[e], full, preferred_element_type=f32)
        weighted = (outputs * gates_ref[e]).astype(bf16)
        slots = lax.dot_general(spread[e], weighted, dims(1, 1), preferred_element_type=f32)
        back[e] = slots.astype(bf16).reshape(N_EP, ROOM, W)
        give.append(
            Exchange(
                lambda p, e=e: back.at[e, p, first],
                lambda p, e=e: returned.at[p, e, first],
                back.at[e, some, first],
                returned.at[some, e, first],
                (back_a, back_b)[e],
            )
        )
        give[e].start()

    way = {1: 0, -1: 1}
    for k in range(1, 5):
        for h, rows in enumerate(cuts):
            for d in (1, -1):
                most = reach(d, h)
                if k > most:
                    continue
                total = term(d * (most + 1 - k), rows)
                if k > 1:
                    link.arrive(got.at[way[d], k - 1, rows], (d, k - 1, h), other)
                    total = total + got[way[d], k - 1, rows].astype(f32)
                made[way[d], k, rows] = total.astype(bf16)
                link.send(
                    made.at[way[d], k, rows],
                    got.at[way[d], k, rows],
                    (d, k, h),
                    z_device(around(z, d, NZ), core),
                )
    for e in range(EXP_DEV):
        give[e].arrive()
    routed = jnp.dot(one_t[...], returned[...].reshape(N_EP * 2 * ROOM, W), preferred_element_type=f32)
    for h, rows in enumerate(cuts):
        total = term(0, rows)
        for d in (1, -1):
            most = reach(d, h)
            link.arrive(got.at[way[d], most, rows], (d, most, h), other)
            total = total + got[way[d], most, rows].astype(f32)
        mixed_ref[rows, :] = (total + routed[h * half : (h + 1) * half]).astype(bf16)
    for one in (ask, *dispatch, *give):
        one.finish()
    for one in (tok_link, *x_links, gu_link, dn_link, hid_link, link):
        one.finish()


def requests_of(chosen):
    sources = chosen // TOK_DEV
    before = jnp.sum((sources[:, None, :] < sources[:, :, None]).astype(i32), axis=2)
    rank = jnp.arange(CAP, dtype=i32)[None, :] - before
    slots = sources * ROOM + rank
    local_ids = chosen - sources * TOK_DEV
    place = (
        jnp.arange(N_EP, dtype=i32)[:, None] * ROOM + jnp.arange(ROOM, dtype=i32)[None, :]
    )
    asked = jnp.max(
        jnp.where(place[None, :, :, None] == slots[:, None, None, :], local_ids[:, None, None, :], -1),
        axis=3,
    )
    asked = jnp.moveaxis(asked, 0, 1).reshape(N_EP, 1, EXP_DEV * ROOM)
    side = lax.rem(lax.axis_index("ep"), 2)
    lane = jnp.arange(W, dtype=i32)
    asked = jnp.where(lane // (W // 2) == side, jnp.concatenate([asked, asked], axis=2), -1)
    return slots, asked


def on_device(
    tokens,
    norm_gain,
    shared_gate,
    shared_up,
    shared_down,
    expert_gate,
    expert_up,
    expert_down,
    chosen,
    gates,
):
    slots, asked = requests_of(chosen)
    gu = jnp.concatenate(
        [shared_gate[:, :W], shared_up[:, :W], shared_gate[:, W:], shared_up[:, W:], jnp.zeros((64, 32), bf16)],
        axis=1,
    )
    dn = jnp.pad(shared_down.T, ((0, 0), (0, 80)))
    vmem = pl.BlockSpec(memory_space=pltpu.VMEM)
    hbm = pl.BlockSpec(memory_space=pl.ANY)
    pool = lambda *shape, dtype=bf16: pltpu.VMEM(shape, dtype)
    dma = lambda n: pltpu.SemaphoreType.DMA((n,))
    return pl.pallas_call(
        layer_kernel,
        name="layer",
        out_shape=jax.ShapeDtypeStruct((TOK_DEV, W), bf16),
        in_specs=[vmem] * 8 + [hbm] * 3,
        out_specs=vmem,
        scratch_shapes=[
            pool(N_EP, 1, W, dtype=i32),
            pool(TOK_DEV, N_EP * 2 * ROOM),
            pool(EXP_DEV, CAP, N_EP * ROOM),
            pool(EXP_DEV, N_EP * ROOM, CAP),
            pool(N_EP, EXP_DEV, ROOM, W),
            pool(EXP_DEV, N_EP, ROOM, W),
            pool(N_TP, TOK_DEV, W),
            pool(EXP_DEV, CAP, W),
            pool(N_TP, EXP_DEV, CAP, W),
            pool(N_EP, 64, 384),
            pool(N_EP, 64, 256),
            pool(F_DEV, CAP),
            pool(N_TP, F_DEV, CAP),
            pool(EXP_DEV, N_EP, ROOM, W),
            pool(N_EP, EXP_DEV, ROOM, W),
            pool(N_TP, TOK_DEV, W),
            pool(NZ, TOK_DEV, W),
            pool(2, 5, TOK_DEV, W),
            pool(2, 5, TOK_DEV, W),
            pool(F_DEV, D),
            pool(F_DEV, D),
            pool(EXP_DEV, F, W),
            pool(EXP_DEV, W, F),
            pool(TOK_DEV, D),
            pool(CAP, D),
            dma(3),
            *[dma(2)] * 5,
            *[dma(32)] * 14,
        ],
        compiler_params=pltpu.CompilerParams(
            collective_id=0, has_side_effects=True, vmem_limit_bytes=56 * 1024 * 1024
        ),
    )(
        asked,
        slots.reshape(EXP_DEV, CAP, 1),
        slots.reshape(EXP_DEV, 1, CAP),
        tokens,
        norm_gain.reshape(1, D),
        gu,
        dn,
        gates.reshape(EXP_DEV, 1, CAP),
        expert_gate.reshape(F_DEV, D),
        expert_up.reshape(F_DEV, D),
        expert_down,
    )


def solution(mesh):
    return jax.shard_map(
        on_device,
        mesh=mesh,
        in_specs=(
            P("ep", "tp"),
            P(),
            P("ep", "tp"),
            P("ep", "tp"),
            P("tp", "ep"),
            P("tp", "ep", None, None),
            P("tp", "ep", None, None),
            P("ep", None, "tp"),
            P("ep", None),
            P("ep", None),
        ),
        out_specs=P("ep", "tp"),
        check_vma=False,
    )
```

```python
import jax
import jax.numpy as jnp
from jax import lax
from jax.experimental import pallas as pl
from jax.experimental.pallas import tpu as pltpu
from jax.sharding import PartitionSpec as P

MESH = pl.DeviceIdType.MESH
EXP_DEV = 2
TOK_DEV = 384
CAP = 384
NZ, NY, NX = 8, 8, 4
N_TP, N_EP = 16, 32
SLOT, ROOM = 24, 32
F_DEV, F = 176, 1408
D, W = 2048, 128
norm_eps = 1e-06
bf16, f32, i32 = jnp.bfloat16, jnp.float32, jnp.int32


class Link:
    def __init__(self, send_sems, recv_sems):
        self.send_sems, self.recv_sems = send_sems, recv_sems
        self.keys, self.sent = {}, []

    def _copy(self, src, dst, key, device):
        i = self.keys.setdefault(key, len(self.keys))
        return pltpu.make_async_remote_copy(
            src_ref=src,
            dst_ref=dst,
            send_sem=self.send_sems.at[i],
            recv_sem=self.recv_sems.at[i],
            device_id=device,
            device_id_type=MESH,
        )

    def send(self, src, dst, key, device):
        copy = self._copy(src, dst, key, device)
        copy.start()
        self.sent.append(copy)

    def arrive(self, dst, key, device):
        self._copy(dst, dst, key, device).wait_recv()

    def finish(self):
        for copy in self.sent:
            copy.wait_send()


def places():
    tp, ep = lax.axis_index("tp"), lax.axis_index("ep")
    return tp // 2, lax.rem(tp, 2), ep // NX, lax.rem(ep, NX)


def around(position, step, count):
    return lax.rem(position + step + count, count)


def z_device(z, core):
    return {"tp": z * 2 + core}


OFFSETS = sorted(
    [(a, b) for a in range(-3, 5) for b in range(-1, 3) if (a, b) != (0, 0)],
    key=lambda o: (o[1] % 4, o[0] % 8),
)


def greet():
    barrier = pltpu.get_barrier_semaphore()
    z, core, y, x = places()
    devices = [{"ep": around(y, a, NY) * NX + around(x, b, NX)} for a, b in OFFSETS]
    devices += [z_device(around(z, 1, NZ), core), z_device(around(z, -1, NZ), core)]
    devices += [z_device(z, 1 - core)]
    for device in devices:
        pl.semaphore_signal(barrier, inc=1, device_id=device, device_id_type=MESH)
    return len(devices)


class Exchange:
    def __init__(self, src, dst, src_all, dst_all, sems):
        self.src, self.dst, self.src_all, self.dst_all, self.sems = src, dst, src_all, dst_all, sems

    def start(self):
        _, _, y, x = places()
        own = y * NX + x
        for a, b in OFFSETS:
            peer = around(y, a, NY) * NX + around(x, b, NX)
            pltpu.make_async_remote_copy(
                src_ref=self.src(peer),
                dst_ref=self.dst(own),
                send_sem=self.sems.at[0],
                recv_sem=self.sems.at[1],
                device_id={"ep": peer},
                device_id_type=MESH,
            ).start()
        self.dst(own)[...] = self.src(own)[...]

    def arrive(self):
        part = self.dst_all
        pltpu.make_async_copy(part, part, self.sems.at[1]).wait()

    def finish(self):
        part = self.src_all
        pltpu.make_async_copy(part, part, self.sems.at[0]).wait()


def reach(direction, flipped):
    return 4 if (direction > 0) != bool(flipped) else 3


def ring_gather(pieces, link):
    z, core, _, _ = places()
    own = z * 2 + core
    other = z_device(z, 1 - core)
    beside = {d: z_device(around(z, d, NZ), core) for d in (1, -1)}
    for h, (flip, src, at) in enumerate(pieces):
        for d in (1, -1):
            link.send(src, at(own), (d, 1, h), beside[d])
    for h, (flip, src, at) in enumerate(pieces):
        link.send(src, at(own), ("core", 0, 0, h), other)
    for flip, src, at in pieces:
        at(own)[...] = src[...]
    yield
    for k in range(1, 5):
        for h, (flip, src, at) in enumerate(pieces):
            for d in (1, -1):
                most = reach(d, flip)
                if k > most:
                    continue
                block = at(around(z, -d * k, NZ) * 2 + core)
                link.arrive(block, (d, k, h), other)
                if k < most:
                    link.send(block, block, (d, k + 1, h), beside[d])
                link.send(block, block, ("core", d, k, h), other)
        yield
    for h, (flip, src, at) in enumerate(pieces):
        link.arrive(at(own + 1 - 2 * core), ("core", 0, 0, h), other)
        for k in range(1, 5):
            for d in (1, -1):
                if k <= reach(d, flip):
                    block = at(around(z, -d * k, NZ) * 2 + 1 - core)
                    link.arrive(block, ("core", d, k, h), other)
    yield


def plane_gather(src, dst, link, y_first):
    _, _, y, x = places()
    a, na, b, nb = (y, NY, x, NX) if y_first else (x, NX, y, NY)

    def index(p, q):
        return p * NX + q if y_first else q * NX + p

    own = index(a, b)
    here = {"ep": own}
    along = {d: {"ep": index(around(a, d, na), b)} for d in (1, -1)}
    across = {d: {"ep": index(a, around(b, d, nb))} for d in (1, -1)}
    for d in (1, -1):
        link.send(src, dst.at[own], ("a", d, 1), along[d])
    dst[own] = src[...]
    yield
    tags = [(0, 0)]
    for k in range(1, na // 2 + 1):
        for d in (1, -1):
            most = na // 2 if d > 0 else na // 2 - 1
            if k > most:
                continue
            tags.append((d, k))
            block = dst.at[index(around(a, -d * k, na), b)]
            link.arrive(block, ("a", d, k), here)
            if k < most:
                link.send(block, block, ("a", d, k + 1), along[d])
            yield
    for n, (d, k) in enumerate(tags):
        block = dst.at[index(around(a, -d * k, na), b)]
        for s in (1, -1):
            link.send(src if n == 0 else block, block, ("b", s, 1, n), across[s])
    yield
    for j in range(1, nb // 2 + 1):
        for n, (d, k) in enumerate(tags):
            for s in (1, -1):
                most = nb // 2 if (s > 0) == (n % 2 == 0) else nb // 2 - 1
                if j > most:
                    continue
                block = dst.at[index(around(a, -d * k, na), around(b, -s * j, nb))]
                link.arrive(block, ("b", s, j, n), here)
                if j < most:
                    link.send(block, block, ("b", s, j + 1, n), across[s])
                yield


def go(job, steps=1000):
    for _ in range(steps):
        if next(job, "end") == "end":
            return


def one_hot(condition):
    return jnp.where(condition, 1.0, 0.0).astype(bf16)


def silu(v):
    return v / (1.0 + jnp.exp(-v))


def dims(a, b):
    return (((a,), (b,)), ((), ()))


def normalise(blocks, gain_ref, out_ref):
    for r in range(0, TOK_DEV, W):
        rows = pl.ds(r, W)
        squares = jnp.zeros((W, W), f32)
        for t in range(N_TP):
            wide = blocks(t)[rows, :].astype(f32)
            squares = squares + wide * wide
        inv = lax.rsqrt(jnp.sum(squares, axis=1, keepdims=True) * (1.0 / D) + norm_eps)
        for t in range(N_TP):
            lanes = slice(t * W, (t + 1) * W)
            wide = blocks(t)[rows, :].astype(f32)
            out_ref[rows, lanes] = (wide * inv * gain_ref[:, lanes]).astype(bf16)


def layer_kernel(
    chosen_ref, tok_ref, gain_ref, sg_ref, su_ref, sd_ref, gates_ref, eg_hbm, eu_hbm, ed_hbm,
    mixed_ref,
    req_ref, gu_ref, dn_ref, wanted, asked, one_t, join, spread, out, came, tok_all, own, rows_all, wg, wd, hid, hid_all, back, returned,
    part, pair, got, made, eg, eu, ed, ed_t, normed, taken,
    load_sem, ask_sem, go_a, go_b, back_a, back_b,
    tok_s, tok_r, xa_s, xa_r, xb_s, xb_r, gu_s, gu_r, dn_s, dn_r, hid_s, hid_r, sum_s, sum_r,
):
    count = greet()
    z, core, _, _ = places()
    other = z_device(z, 1 - core)
    loads = [
        pltpu.make_async_copy(s, d, load_sem.at[i])
        for i, (s, d) in enumerate(((eg_hbm, eg), (eu_hbm, eu), (ed_hbm, ed)))
    ]
    for load in loads:
        load.start()
    gu_ref[:, :W] = sg_ref[:, :W]
    gu_ref[:, W : 2 * W] = su_ref[:, :W]
    gu_ref[:, 2 * W :] = jnp.concatenate(
        [sg_ref[:, W:], su_ref[:, W:], jnp.zeros((64, 32), bf16)], axis=1
    )
    dn_ref[...] = jnp.concatenate([sd_ref[...], jnp.zeros((64, 80), bf16)], axis=1)
    came[...] = jnp.zeros_like(came)
    returned[...] = jnp.zeros_like(returned)
    slot_rows = []
    lane = lax.broadcasted_iota(i32, (CAP, W), 1)
    for e in range(EXP_DEV):
        ids = chosen_ref[e : e + 1, :]
        sources = owner_of(ids)
        ids_down = jnp.broadcast_to(ids, (W, CAP)).T
        sources_down = owner_of(ids_down)
        before = jnp.sum(
            jnp.where(jnp.concatenate([sources_down] * 3, axis=1) < sources, 1, 0), axis=0, keepdims=True
        )
        slots = sources * ROOM + lax.broadcasted_iota(i32, (1, CAP), 1) - before
        slot_rows.append(slots)
        slots_down = jnp.broadcast_to(slots, (W, CAP)).T
        local = ids_down - sources_down * TOK_DEV
        for b in range(N_EP * ROOM // W):
            match = slots_down == lane + b * W
            join[e, :, b * W : (b + 1) * W] = one_hot(match)
            wanted[e, b : b + 1] = jnp.max(jnp.where(match, local, -1), axis=0, keepdims=True)
    side = lax.rem(lax.axis_index("ep"), 2)
    lane = lax.broadcasted_iota(i32, (NY, W), 1)
    for i in range(NX):
        a, b = (pltpu.roll(wanted[e], (e - i) % NX * ROOM, 1) for e in range(EXP_DEV))
        both = jnp.where(lane < ROOM, a, jnp.where(lane < 2 * ROOM, b, -1))
        both = jnp.where(side == 0, both, pltpu.roll(both, W // 2, 1))
        for j in range(NY):
            req_ref[j * NX + i] = both[j : j + 1]
    pl.semaphore_wait(pltpu.get_barrier_semaphore(), count)

    half = TOK_DEV // 2
    cuts = [pl.ds(0, half), pl.ds(half, half)]
    first = pl.ds(0, SLOT)
    some = pl.ds(0, N_EP - 1)

    ask = Exchange(
        lambda p: req_ref.at[p], lambda p: asked.at[p], req_ref.at[some], asked.at[some], ask_sem
    )
    ask.start()
    tok_link = Link(tok_s, tok_r)
    tok_ring = ring_gather(
        [(h, tok_ref.at[c], lambda t, c=c: tok_all.at[t, c]) for h, c in enumerate(cuts)], tok_link
    )
    go(tok_ring, 1)
    gu_link, dn_link = Link(gu_s, gu_r), Link(dn_s, dn_r)
    gu_job = plane_gather(gu_ref, wg, gu_link, True)
    dn_job = plane_gather(dn_ref, wd, dn_link, False)
    go(gu_job, 1)
    go(dn_job, 1)
    for e in range(EXP_DEV):
        at = lax.broadcasted_iota(i32, (N_EP * ROOM, CAP), 0)
        spread[e] = one_hot(at == slot_rows[e])
    go(tok_ring, 1)
    go(gu_job, 2)
    go(dn_job, 2)

    ask.arrive()
    token = lax.broadcasted_iota(i32, (TOK_DEV, W), 0)
    for i in range(N_EP // 2):
        ids = jnp.maximum(asked[2 * i], asked[2 * i + 1])
        one_t[:, i * W : (i + 1) * W] = one_hot(token == ids)
    for i in range(4):
        lanes = slice(i * 512, (i + 1) * 512)
        picked = lax.dot_general(
            one_t[:, lanes], tok_ref[...], dims(0, 0), preferred_element_type=f32
        )
        out[i * 8 : (i + 1) * 8] = picked.astype(bf16).reshape(8, EXP_DEV, ROOM, W)
    dispatch = [
        Exchange(
            lambda p, e=e: out.at[p, e, first],
            lambda p, e=e: came.at[e, p, first],
            out.at[some, e, first],
            came.at[e, some, first],
            sem,
        )
        for e, sem in enumerate((go_a, go_b))
    ]
    for e in range(EXP_DEV):
        dispatch[e].start()
    go(tok_ring, 1)
    go(gu_job, 2)
    go(dn_job, 1)
    for load in loads:
        load.wait()
    for e in range(EXP_DEV):
        ed_t[e] = ed[e].T
    go(tok_ring, 1)
    go(gu_job, 2)

    x_links = [Link(xa_s, xa_r), Link(xb_s, xb_r)]
    x_rings = []
    for e in range(EXP_DEV):
        dispatch[e].arrive()
        own[e] = jnp.dot(
            join[e], came[e].reshape(N_EP * ROOM, W), preferred_element_type=f32
        ).astype(bf16)
        x_rings.append(
            ring_gather(
                [
                    (e + h, own.at[e, c], lambda t, c=c, e=e: rows_all.at[t, e, c])
                    for h, c in enumerate(cuts)
                ],
                x_links[e],
            )
        )
        go(x_rings[e], 1)
    go(tok_ring)
    go(gu_job, 2)
    go(dn_job, 1)
    for k in range(4):
        for e in range(EXP_DEV):
            go(x_rings[e], 1)
        if k > 0:
            go(gu_job, 6)
            go(dn_job, 6)
    for e in range(EXP_DEV):
        go(x_rings[e], 1)

    expert = z // (NZ // EXP_DEV)
    normalise(lambda t: rows_all.at[t, expert], gain_ref, taken)
    gate_values = lax.dot_general(eg[...], taken[...], dims(1, 1), preferred_element_type=f32)
    up_values = lax.dot_general(eu[...], taken[...], dims(1, 1), preferred_element_type=f32)
    hid[...] = (silu(gate_values) * up_values).astype(bf16)
    hid_link = Link(hid_s, hid_r)
    hid_ring = ring_gather(
        [
            (h, hid.at[c], lambda t, c=c: hid_all.at[t, c])
            for h, c in enumerate((pl.ds(0, 96), pl.ds(96, 80)))
        ],
        hid_link,
    )
    go(hid_ring, 1)

    normalise(lambda t: tok_all.at[t], gain_ref, normed)
    go(hid_ring, 1)
    go(gu_job)
    sums = jnp.dot(normed[...], wg[...].reshape(D, 384), preferred_element_type=f32)
    low = silu(sums[:, :W]) * sums[:, W : 2 * W]
    high = silu(sums[:, 256:304]) * sums[:, 304:352]
    shared = jnp.concatenate([low, high, jnp.zeros((TOK_DEV, 80), f32)], axis=1).astype(bf16)
    go(hid_ring, 1)
    go(dn_job)
    for t in range(N_TP):
        block = lax.dot_general(
            shared, wd[2 * t : 2 * t + 2].reshape(W, 256), dims(1, 1), preferred_element_type=f32
        )
        part[t] = block.astype(bf16)
    go(hid_ring, 1)

    link = Link(sum_s, sum_r)
    order = [4, -3, 3, -2, 2, -1, 1, 0]
    targets = {m % NZ: around(z, m, NZ) for m in order}
    for m in order:
        at = targets[m % NZ]
        link.send(part.at[at * 2 + 1 - core], pair.at[at], ("core", m % NZ), other)
    here = set()

    def term(m, rows):
        m = m % NZ
        at = targets[m]
        if m not in here:
            link.arrive(pair.at[at], ("core", m), other)
            here.add(m)
        return part[at * 2 + core, rows].astype(f32) + pair[at, rows].astype(f32)

    go(hid_ring)

    give = []
    for e in range(EXP_DEV):
        full = hid_all[e * 8 : (e + 1) * 8].reshape(F, CAP)
        outputs = jnp.dot(ed_t[e], full, preferred_element_type=f32)
        weighted = (outputs * gates_ref[e : e + 1, :]).astype(bf16)
        slots = lax.dot_general(spread[e], weighted, dims(1, 1), preferred_element_type=f32)
        back[e] = slots.astype(bf16).reshape(N_EP, ROOM, W)
        give.append(
            Exchange(
                lambda p, e=e: back.at[e, p, first],
                lambda p, e=e: returned.at[p, e, first],
                back.at[e, some, first],
                returned.at[some, e, first],
                (back_a, back_b)[e],
            )
        )
        give[e].start()

    way = {1: 0, -1: 1}
    for k in range(1, 5):
        for h, rows in enumerate(cuts):
            for d in (1, -1):
                most = reach(d, h)
                if k > most:
                    continue
                total = term(d * (most + 1 - k), rows)
                if k > 1:
                    link.arrive(got.at[way[d], k - 1, rows], (d, k - 1, h), other)
                    total = total + got[way[d], k - 1, rows].astype(f32)
                made[way[d], k, rows] = total.astype(bf16)
                link.send(
                    made.at[way[d], k, rows],
                    got.at[way[d], k, rows],
                    (d, k, h),
                    z_device(around(z, d, NZ), core),
                )
    for e in range(EXP_DEV):
        give[e].arrive()
    routed = jnp.dot(one_t[...], returned[...].reshape(N_EP * 2 * ROOM, W), preferred_element_type=f32)
    for h, rows in enumerate(cuts):
        total = term(0, rows)
        for d in (1, -1):
            most = reach(d, h)
            link.arrive(got.at[way[d], most, rows], (d, most, h), other)
            total = total + got[way[d], most, rows].astype(f32)
        mixed_ref[rows, :] = total + routed[h * half : (h + 1) * half]
    for one in (ask, *dispatch, *give):
        one.finish()
    for one in (tok_link, *x_links, gu_link, dn_link, hid_link, link):
        one.finish()


def owner_of(ids):
    return ((ids >> 7) * 171) >> 9


def on_device(
    tokens,
    norm_gain,
    shared_gate,
    shared_up,
    shared_down,
    expert_gate,
    expert_up,
    expert_down,
    chosen,
    gates,
):
    vmem = pl.BlockSpec(memory_space=pltpu.VMEM)
    hbm = pl.BlockSpec(memory_space=pl.ANY)
    pool = lambda *shape, dtype=bf16: pltpu.VMEM(shape, dtype)
    dma = lambda n: pltpu.SemaphoreType.DMA((n,))
    return pl.pallas_call(
        layer_kernel,
        name="layer",
        out_shape=jax.ShapeDtypeStruct((TOK_DEV, W), f32),
        in_specs=[vmem] * 7 + [hbm] * 3,
        out_specs=vmem,
        scratch_shapes=[
            pool(N_EP, 1, W, dtype=i32),
            pool(64, 384),
            pool(64, 256),
            pool(EXP_DEV, NY, W, dtype=i32),
            pool(N_EP, 1, W, dtype=i32),
            pool(TOK_DEV, N_EP * 2 * ROOM),
            pool(EXP_DEV, CAP, N_EP * ROOM),
            pool(EXP_DEV, N_EP * ROOM, CAP),
            pool(N_EP, EXP_DEV, ROOM, W),
            pool(EXP_DEV, N_EP, ROOM, W),
            pool(N_TP, TOK_DEV, W),
            pool(EXP_DEV, CAP, W),
            pool(N_TP, EXP_DEV, CAP, W),
            pool(N_EP, 64, 384),
            pool(N_EP, 64, 256),
            pool(F_DEV, CAP),
            pool(N_TP, F_DEV, CAP),
            pool(EXP_DEV, N_EP, ROOM, W),
            pool(N_EP, EXP_DEV, ROOM, W),
            pool(N_TP, TOK_DEV, W),
            pool(NZ, TOK_DEV, W),
            pool(2, 5, TOK_DEV, W),
            pool(2, 5, TOK_DEV, W),
            pool(F_DEV, D),
            pool(F_DEV, D),
            pool(EXP_DEV, F, W),
            pool(EXP_DEV, W, F),
            pool(TOK_DEV, D),
            pool(CAP, D),
            dma(3),
            *[dma(2)] * 5,
            *[dma(32)] * 14,
        ],
        compiler_params=pltpu.CompilerParams(
            collective_id=0, has_side_effects=True, vmem_limit_bytes=56 * 1024 * 1024
        ),
    )(
        chosen,
        tokens,
        norm_gain.reshape(1, D),
        shared_gate,
        shared_up,
        shared_down.T,
        gates,
        expert_gate.reshape(F_DEV, D),
        expert_up.reshape(F_DEV, D),
        expert_down,
    ).astype(bf16)


def solution(mesh):
    return jax.shard_map(
        on_device,
        mesh=mesh,
        in_specs=(
            P("ep", "tp"),
            P(),
            P("ep", "tp"),
            P("ep", "tp"),
            P("tp", "ep"),
            P("tp", "ep", None, None),
            P("tp", "ep", None, None),
            P("ep", None, "tp"),
            P("ep", None),
            P("ep", None),
        ),
        out_specs=P("ep", "tp"),
        check_vma=False,
    )
```

```python
import jax
import jax.numpy as jnp
from jax import lax
from jax.experimental import pallas as pl
from jax.experimental.pallas import tpu as pltpu
from jax.sharding import PartitionSpec as P

MESH = pl.DeviceIdType.MESH
EXP_DEV = 2
TOK_DEV = 384
CAP = 384
NZ, NY, NX = 8, 8, 4
N_TP, N_EP = 16, 32
SLOT, ROOM = 24, 32
F_DEV, F = 176, 1408
D, W = 2048, 128
norm_eps = 1e-06
bf16, f32, i32 = jnp.bfloat16, jnp.float32, jnp.int32


class Link:
    def __init__(self, send_sems, recv_sems):
        self.send_sems, self.recv_sems = send_sems, recv_sems
        self.keys, self.sent = {}, {None: [], 0: [], 1: []}

    def _copy(self, src, dst, key, device):
        i = self.keys.setdefault(key, len(self.keys))
        return pltpu.make_async_remote_copy(
            src_ref=src,
            dst_ref=dst,
            send_sem=self.send_sems.at[i],
            recv_sem=self.recv_sems.at[i],
            device_id=device,
            device_id_type=MESH,
        )

    def send(self, copy, core=None):
        self._copy(*copy()).start()
        self.sent[core].append(copy)

    def arrive(self, dst, key, device):
        self._copy(dst, dst, key, device).wait_recv()

    def finish(self):
        for copy in self.sent[None]:
            self._copy(*copy()).wait_send()
        for core in (0, 1):

            @on_core(core)
            def _(core=core):
                for copy in self.sent[core]:
                    self._copy(*copy()).wait_send()


def on_core(core):
    return pl.when(lax.rem(lax.axis_index("tp"), 2) == core)


def places():
    tp, ep = lax.axis_index("tp"), lax.axis_index("ep")
    return tp // 2, lax.rem(tp, 2), ep // NX, lax.rem(ep, NX)


def around(position, step, count):
    return lax.rem(position + step + count, count)


def z_device(z, core):
    return {"tp": z * 2 + core}


OFFSETS = sorted(
    [(a, b) for a in range(-3, 5) for b in range(-1, 3) if (a, b) != (0, 0)],
    key=lambda o: (o[1] % 4, o[0] % 8),
)


def greet():
    barrier = pltpu.get_barrier_semaphore()
    z, core, y, x = places()
    devices = [{"ep": around(y, a, NY) * NX + around(x, b, NX)} for a, b in OFFSETS]
    devices += [z_device(around(z, 1, NZ), core), z_device(around(z, -1, NZ), core)]
    devices += [z_device(z, 1 - core)]
    for device in devices:
        pl.semaphore_signal(barrier, inc=1, device_id=device, device_id_type=MESH)
    return len(devices)


class Exchange:
    def __init__(self, src, dst, src_all, dst_all, sems):
        self.src, self.dst, self.src_all, self.dst_all, self.sems = src, dst, src_all, dst_all, sems

    def start(self):
        _, _, y, x = places()
        own = y * NX + x
        for a, b in OFFSETS:
            peer = around(y, a, NY) * NX + around(x, b, NX)
            pltpu.make_async_remote_copy(
                src_ref=self.src(peer),
                dst_ref=self.dst(own),
                send_sem=self.sems.at[0],
                recv_sem=self.sems.at[1],
                device_id={"ep": peer},
                device_id_type=MESH,
            ).start()
        self.dst(own)[...] = self.src(own)[...]

    def arrive(self):
        part = self.dst_all
        pltpu.make_async_copy(part, part, self.sems.at[1]).wait()

    def finish(self):
        part = self.src_all
        pltpu.make_async_copy(part, part, self.sems.at[0]).wait()


def reach(direction, flipped):
    return 4 if (direction > 0) != bool(flipped) else 3


def ring_gather(pieces, link):
    def place():
        return lax.axis_index("tp") // 2

    def beside(d):
        return z_device(around(place(), d, NZ), 1)

    def mate(core):
        return z_device(place(), core)

    numbered = list(enumerate(pieces))
    order = [(c, h, (flip + c) % 2, at) for c in (1, 0) for h, (flip, src, at) in numbered]

    @on_core(1)
    def _():
        for h, (flip, src, at) in numbered:
            for d in (1, -1):
                link.send(lambda h=h, src=src, at=at, d=d: (src, at(place() * 2 + 1), (d, 1, h, 1), beside(d)), 1)
        for h, (flip, src, at) in numbered:
            link.send(lambda h=h, src=src, at=at: (src, at(place() * 2 + 1), ("core", 0, 0, h, 1), mate(0)), 1)

    @on_core(0)
    def _():
        for h, (flip, src, at) in numbered:
            link.send(lambda h=h, src=src, at=at: (src, at(place() * 2), ("core", 0, 0, h, 0), mate(1)), 0)

    for flip, src, at in pieces:
        at(lax.axis_index("tp"))[...] = src[...]

    @on_core(1)
    def _():
        for h, (flip, src, at) in numbered:
            block = lambda at=at: at(place() * 2)
            link.arrive(block(), ("core", 0, 0, h, 0), mate(0))
            for d in (1, -1):
                link.send(lambda h=h, b=block, d=d: (b(), b(), (d, 1, h, 0), beside(d)), 1)

    yield
    for k in range(1, 5):

        @on_core(1)
        def _(k=k):
            for c, h, flip, at in order:
                for d in (1, -1):
                    most = reach(d, flip)
                    if k > most:
                        continue
                    block = lambda at=at, d=d, c=c: at(around(place(), -d * k, NZ) * 2 + c)
                    link.arrive(block(), (d, k, h, c), mate(0))
                    if k < most:
                        link.send(lambda b=block, d=d, h=h, c=c: (b(), b(), (d, k + 1, h, c), beside(d)), 1)
                    link.send(lambda b=block, d=d, h=h, c=c: (b(), b(), ("core", d, k, h, c), mate(0)), 1)

        yield

    @on_core(0)
    def _():
        for h, (flip, src, at) in numbered:
            link.arrive(at(place() * 2 + 1), ("core", 0, 0, h, 1), mate(1))
        for k in range(1, 5):
            for c, h, flip, at in order:
                for d in (1, -1):
                    if k <= reach(d, flip):
                        link.arrive(at(around(place(), -d * k, NZ) * 2 + c), ("core", d, k, h, c), mate(1))

    yield


def plane_gather(src, dst, link, y_first):
    na, nb = (NY, NX) if y_first else (NX, NY)

    def at(da=0, db=0):
        _, _, y, x = places()
        if y_first:
            return around(y, da, NY) * NX + around(x, db, NX)
        return around(y, db, NY) * NX + around(x, da, NX)

    def mate(core):
        return z_device(places()[0], core)

    def send(key, da, db, block):
        link.send(lambda: (block(), block(), key, {"ep": at(da, db)}), 0)

    @on_core(1)
    def _():
        link.send(lambda: (src, dst.at[at(), 1], ("in",), mate(0)), 1)

    dst[at(), lax.rem(lax.axis_index("tp"), 2)] = src[...]
    yield

    @on_core(0)
    def _():
        link.arrive(dst.at[at(), 1], ("in",), mate(1))
        for d in (1, -1):
            send(("a", d, 1), d, 0, lambda: dst.at[at()])
        for s in (1, -1):
            send(("b", s, 1, 0), 0, s, lambda: dst.at[at()])

    yield
    tags = [(0, 0)]
    to_one = []

    def share(block, key):
        to_one.append((block, key))
        link.send(lambda: (block().at[1], block().at[1], key, mate(1)), 0)

    for k in range(1, na // 2 + 1):
        for d in (1, -1):
            most = na // 2 if d > 0 else na // 2 - 1
            if k > most:
                continue
            block = lambda d=d, k=k: dst.at[at(-d * k, 0)]

            @on_core(0)
            def _(d=d, k=k, block=block):
                link.arrive(block(), ("a", d, k), {"ep": at()})
                if k < most:
                    send(("a", d, k + 1), d, 0, block)
                for s in (1, -1):
                    send(("b", s, 1, len(tags)), 0, s, block)
                share(block, ("one", len(to_one)))

            tags.append((d, k))
            yield
    for j in range(1, nb // 2 + 1):
        for n, (d, k) in enumerate(tags):
            for s in (1, -1):
                most = nb // 2 if (s > 0) == (n % 2 == 0) else nb // 2 - 1
                if j > most:
                    continue
                block = lambda d=d, k=k, s=s, j=j: dst.at[at(-d * k, -s * j)]

                @on_core(0)
                def _(s=s, j=j, n=n, block=block):
                    link.arrive(block(), ("b", s, j, n), {"ep": at()})
                    if j < most:
                        send(("b", s, j + 1, n), 0, s, block)
                    share(block, ("one", len(to_one)))

                yield

    @on_core(1)
    def _():
        for block, key in to_one:
            link.arrive(block().at[1], key, mate(0))

    yield


def go(job, steps=1000):
    for _ in range(steps):
        if next(job, "end") == "end":
            return


def one_hot(condition):
    return jnp.where(condition, 1.0, 0.0).astype(bf16)


def silu(v):
    return v / (1.0 + jnp.exp(-v))


def dims(a, b):
    return (((a,), (b,)), ((), ()))


def normalise(blocks, gain_ref, out_ref):
    for r in range(0, TOK_DEV, W):
        rows = pl.ds(r, W)
        squares = jnp.zeros((W, W), f32)
        for t in range(N_TP):
            wide = blocks(t)[rows, :].astype(f32)
            squares = squares + wide * wide
        inv = lax.rsqrt(jnp.sum(squares, axis=1, keepdims=True) * (1.0 / D) + norm_eps)
        for t in range(N_TP):
            lanes = slice(t * W, (t + 1) * W)
            wide = blocks(t)[rows, :].astype(f32)
            out_ref[rows, lanes] = (wide * inv * gain_ref[:, lanes]).astype(bf16)


def layer_kernel(
    chosen_hbm, sg_hbm, su_hbm, sd_hbm, tok_hbm, gain_hbm, gates_hbm, eg_hbm, eu_hbm, ed_hbm,
    mixed_ref,
    chosen_ref, sg_ref, su_ref, sd_ref, tok_ref, gain_ref, gates_ref,
    req_ref, gu_ref, dn_ref, wanted, asked, one_t, join, spread, out, came, tok_all, own, rows_all, wg, wd, hid, hid_all, back, returned,
    part, pair, got, made, eg, eu, ed, ed_t, normed, taken,
    load_sem, ask_sem, go_a, go_b, back_a, back_b,
    tok_s, tok_r, xa_s, xa_r, xb_s, xb_r, gu_s, gu_r, dn_s, dn_r, hid_s, hid_r, sum_s, sum_r,
):
    count = greet()
    z, core, _, _ = places()
    other = z_device(z, 1 - core)
    loads = [
        pltpu.make_async_copy(s, d, load_sem.at[i])
        for i, (s, d) in enumerate(
            (
                (chosen_hbm, chosen_ref),
                (sg_hbm, sg_ref),
                (su_hbm, su_ref),
                (sd_hbm, sd_ref),
                (tok_hbm, tok_ref),
                (gain_hbm, gain_ref),
                (gates_hbm, gates_ref),
                (eg_hbm, eg),
                (eu_hbm, eu),
                (ed_hbm, ed),
            )
        )
    ]
    for load in loads:
        load.start()
    for load in loads[:4]:
        load.wait()
    gu_ref[:, :W] = sg_ref[:, :W]
    gu_ref[:, W : 2 * W] = su_ref[:, :W]
    gu_ref[:, 2 * W :] = jnp.concatenate(
        [sg_ref[:, W:], su_ref[:, W:], jnp.zeros((64, 32), bf16)], axis=1
    )
    dn_ref[...] = jnp.concatenate([sd_ref[...], jnp.zeros((64, 80), bf16)], axis=1)
    came[...] = jnp.zeros_like(came)
    returned[...] = jnp.zeros_like(returned)
    slot_rows = []
    lane = lax.broadcasted_iota(i32, (CAP, W), 1)
    for e in range(EXP_DEV):
        ids = chosen_ref[e : e + 1, :]
        sources = owner_of(ids)
        ids_down = jnp.broadcast_to(ids, (W, CAP)).T
        sources_down = owner_of(ids_down)
        before = jnp.sum(
            jnp.where(jnp.concatenate([sources_down] * 3, axis=1) < sources, 1, 0), axis=0, keepdims=True
        )
        slots = sources * ROOM + lax.broadcasted_iota(i32, (1, CAP), 1) - before
        slot_rows.append(slots)
        slots_down = jnp.broadcast_to(slots, (W, CAP)).T
        local = ids_down - sources_down * TOK_DEV
        for b in range(N_EP * ROOM // W):
            match = slots_down == lane + b * W
            join[e, :, b * W : (b + 1) * W] = one_hot(match)
            wanted[e, b : b + 1] = jnp.max(jnp.where(match, local, -1), axis=0, keepdims=True)
    side = lax.rem(lax.axis_index("ep"), 2)
    lane = lax.broadcasted_iota(i32, (NY, W), 1)
    for i in range(NX):
        a, b = (pltpu.roll(wanted[e], (e - i) % NX * ROOM, 1) for e in range(EXP_DEV))
        both = jnp.where(lane < ROOM, a, jnp.where(lane < 2 * ROOM, b, -1))
        both = jnp.where(side == 0, both, pltpu.roll(both, W // 2, 1))
        for j in range(NY):
            req_ref[j * NX + i] = both[j : j + 1]
    loads[4].wait()
    pl.semaphore_wait(pltpu.get_barrier_semaphore(), count)

    half = TOK_DEV // 2
    cuts = [pl.ds(0, half), pl.ds(half, half)]
    first = pl.ds(0, SLOT)
    some = pl.ds(0, N_EP - 1)

    half = TOK_DEV // 2
    cuts = [pl.ds(0, half), pl.ds(half, half)]
    first = pl.ds(0, SLOT)
    some = pl.ds(0, N_EP - 1)
    ask = Exchange(
        lambda p: req_ref.at[p], lambda p: asked.at[p], req_ref.at[some], asked.at[some], ask_sem
    )
    ask.start()
    tok_link = Link(tok_s, tok_r)
    tok_ring = ring_gather(
        [(h, tok_ref.at[c], lambda t, c=c: tok_all.at[t, c]) for h, c in enumerate(cuts)], tok_link
    )
    go(tok_ring, 1)
    gu_link, dn_link = Link(gu_s, gu_r), Link(dn_s, dn_r)
    gu_job = plane_gather(gu_ref, wg, gu_link, True)
    dn_job = plane_gather(dn_ref, wd, dn_link, False)
    go(gu_job, 1)
    go(dn_job, 1)
    for e in range(EXP_DEV):
        at = lax.broadcasted_iota(i32, (N_EP * ROOM, CAP), 0)
        spread[e] = one_hot(at == slot_rows[e])
    go(tok_ring, 1)

    ask.arrive()
    token = lax.broadcasted_iota(i32, (TOK_DEV, W), 0)
    for i in range(N_EP // 2):
        ids = jnp.maximum(asked[2 * i], asked[2 * i + 1])
        one_t[:, i * W : (i + 1) * W] = one_hot(token == ids)
    for i in range(4):
        lanes = slice(i * 512, (i + 1) * 512)
        picked = lax.dot_general(
            one_t[:, lanes], tok_ref[...], dims(0, 0), preferred_element_type=f32
        )
        out[i * 8 : (i + 1) * 8] = picked.astype(bf16).reshape(8, EXP_DEV, ROOM, W)
    dispatch = [
        Exchange(
            lambda p, e=e: out.at[p, e, first],
            lambda p, e=e: came.at[e, p, first],
            out.at[some, e, first],
            came.at[e, some, first],
            sem,
        )
        for e, sem in enumerate((go_a, go_b))
    ]
    for e in range(EXP_DEV):
        dispatch[e].start()
    for load in loads[5:]:
        load.wait()
    for e in range(EXP_DEV):
        ed_t[e] = ed[e].T
    go(tok_ring, 1)
    go(tok_ring, 1)

    x_links = [Link(xa_s, xa_r), Link(xb_s, xb_r)]
    x_rings = []
    for e in range(EXP_DEV):
        dispatch[e].arrive()
        own[e] = jnp.dot(
            join[e], came[e].reshape(N_EP * ROOM, W), preferred_element_type=f32
        ).astype(bf16)
        x_rings.append(
            ring_gather(
                [
                    (e + h, own.at[e, c], lambda t, c=c, e=e: rows_all.at[t, e, c])
                    for h, c in enumerate(cuts)
                ],
                x_links[e],
            )
        )
        go(x_rings[e], 1)
        if e == 0:
            go(tok_ring, 1)
    for k in range(13):
        go(gu_job, 1)
        go(dn_job, 1)
    for k in range(4):
        for e in range(EXP_DEV):
            go(x_rings[e], 1)
    for e in range(EXP_DEV):
        go(x_rings[e], 1)

    expert = z // (NZ // EXP_DEV)
    normalise(lambda t: rows_all.at[t, expert], gain_ref, taken)
    gate_values = lax.dot_general(eg[...], taken[...], dims(1, 1), preferred_element_type=f32)
    up_values = lax.dot_general(eu[...], taken[...], dims(1, 1), preferred_element_type=f32)
    hid[...] = (silu(gate_values) * up_values).astype(bf16)
    hid_link = Link(hid_s, hid_r)
    hid_ring = ring_gather(
        [
            (h, hid.at[c], lambda t, c=c: hid_all.at[t, c])
            for h, c in enumerate((pl.ds(0, 96), pl.ds(96, 80)))
        ],
        hid_link,
    )
    go(hid_ring, 1)

    for k in range(18):
        go(gu_job, 1)
        go(dn_job, 1)
    go(tok_ring)
    normalise(lambda t: tok_all.at[t], gain_ref, normed)
    go(hid_ring, 1)
    go(hid_ring, 1)
    go(gu_job)
    mine = pl.ds(core, 1)
    weights = wg[:, mine].reshape(D, 384)
    sums = jnp.dot(normed[...], weights, preferred_element_type=f32)
    low = silu(sums[:, :W]) * sums[:, W : 2 * W]
    high = silu(sums[:, 256:304]) * sums[:, 304:352]
    shared = jnp.concatenate([low, high, jnp.zeros((TOK_DEV, 80), f32)], axis=1).astype(bf16)
    go(hid_ring, 1)
    go(dn_job)
    link = Link(sum_s, sum_r)
    for t in range(N_TP):
        weights = wd[2 * t : 2 * t + 2, mine].reshape(W, 256)
        block = lax.dot_general(shared, weights, dims(1, 1), preferred_element_type=f32)
        part[t] = block.astype(bf16)
        if t % 2:
            i = t // 2
            link.send(lambda i=i: (part.at[2 * i + 1 - core], pair.at[i], ("core", i), other))
    for i in range(NZ):
        link.arrive(pair.at[i], ("core", i), other)

    way = {1: 0, -1: 1}

    def term(m, rows):
        at = around(z, m, NZ)
        return part[at * 2 + core, rows].astype(f32) + pair[at, rows].astype(f32)

    def sum_round(k):
        for h, rows in enumerate(cuts):
            for d in (1, -1):
                most = reach(d, h)
                if k > most:
                    continue
                total = term(d * (most + 1 - k), rows)
                if k > 1:
                    link.arrive(got.at[way[d], k - 1, rows], (d, k - 1, h), other)
                    total = total + got[way[d], k - 1, rows].astype(f32)
                made[way[d], k, rows] = total.astype(bf16)
                src, dst = made.at[way[d], k, rows], got.at[way[d], k, rows]
                beside = z_device(around(z, d, NZ), core)
                link.send(lambda s=src, t=dst, d=d, h=h, b=beside: (s, t, (d, k, h), b))

    sum_round(1)
    go(hid_ring, 1)
    go(hid_ring)

    give = []
    for e in range(EXP_DEV):
        full = hid_all[e * 8 : (e + 1) * 8].reshape(F, CAP)
        outputs = jnp.dot(ed_t[e], full, preferred_element_type=f32)
        weighted = (outputs * gates_ref[e : e + 1, :]).astype(bf16)
        slots = lax.dot_general(spread[e], weighted, dims(1, 1), preferred_element_type=f32)
        back[e] = slots.astype(bf16).reshape(N_EP, ROOM, W)
        give.append(
            Exchange(
                lambda p, e=e: back.at[e, p, first],
                lambda p, e=e: returned.at[p, e, first],
                back.at[e, some, first],
                returned.at[some, e, first],
                (back_a, back_b)[e],
            )
        )
        give[e].start()

    for k in range(2, 5):
        sum_round(k)
    for h, rows in enumerate(cuts):
        total = term(0, rows)
        for d in (1, -1):
            most = reach(d, h)
            link.arrive(got.at[way[d], most, rows], (d, most, h), other)
            total = total + got[way[d], most, rows].astype(f32)
        mixed_ref[rows, :] = total
    for e in range(EXP_DEV):
        give[e].arrive()
    mixed_ref[...] += jnp.dot(
        one_t[...], returned[...].reshape(N_EP * 2 * ROOM, W), preferred_element_type=f32
    )
    for one in (ask, *dispatch, *give):
        one.finish()
    for one in (tok_link, *x_links, gu_link, dn_link, hid_link, link):
        one.finish()


def owner_of(ids):
    return ((ids >> 7) * 171) >> 9


def on_device(
    tokens,
    norm_gain,
    shared_gate,
    shared_up,
    shared_down,
    expert_gate,
    expert_up,
    expert_down,
    chosen,
    gates,
):
    vmem = pl.BlockSpec(memory_space=pltpu.VMEM)
    hbm = pl.BlockSpec(memory_space=pltpu.HBM)
    pool = lambda *shape, dtype=bf16: pltpu.VMEM(shape, dtype)
    dma = lambda n: pltpu.SemaphoreType.DMA((n,))
    return pl.pallas_call(
        layer_kernel,
        name="layer",
        out_shape=jax.ShapeDtypeStruct((TOK_DEV, W), f32),
        in_specs=[hbm] * 10,
        out_specs=vmem,
        scratch_shapes=[
            pool(EXP_DEV, CAP, dtype=i32),
            pool(64, F_DEV),
            pool(64, F_DEV),
            pool(64, F_DEV),
            pool(TOK_DEV, W),
            pool(1, D, dtype=f32),
            pool(EXP_DEV, CAP, dtype=f32),
            pool(N_EP, 1, W, dtype=i32),
            pool(64, 384),
            pool(64, 256),
            pool(EXP_DEV, NY, W, dtype=i32),
            pool(N_EP, 1, W, dtype=i32),
            pool(TOK_DEV, N_EP * 2 * ROOM),
            pool(EXP_DEV, CAP, N_EP * ROOM),
            pool(EXP_DEV, N_EP * ROOM, CAP),
            pool(N_EP, EXP_DEV, ROOM, W),
            pool(EXP_DEV, N_EP, ROOM, W),
            pool(N_TP, TOK_DEV, W),
            pool(EXP_DEV, CAP, W),
            pool(N_TP, EXP_DEV, CAP, W),
            pool(N_EP, 2, 64, 384),
            pool(N_EP, 2, 64, 256),
            pool(F_DEV, CAP),
            pool(N_TP, F_DEV, CAP),
            pool(EXP_DEV, N_EP, ROOM, W),
            pool(N_EP, EXP_DEV, ROOM, W),
            pool(N_TP, TOK_DEV, W),
            pool(NZ, TOK_DEV, W),
            pool(2, 5, TOK_DEV, W),
            pool(2, 5, TOK_DEV, W),
            pool(F_DEV, D),
            pool(F_DEV, D),
            pool(EXP_DEV, F, W),
            pool(EXP_DEV, W, F),
            pool(TOK_DEV, D),
            pool(CAP, D),
            dma(10),
            *[dma(2)] * 5,
            *[dma(64)] * 12,
            *[dma(32)] * 2,
        ],
        compiler_params=pltpu.CompilerParams(
            collective_id=0, has_side_effects=True, vmem_limit_bytes=56 * 1024 * 1024
        ),
    )(
        chosen,
        shared_gate,
        shared_up,
        shared_down.T,
        tokens,
        norm_gain.reshape(1, D),
        gates,
        expert_gate.reshape(F_DEV, D),
        expert_up.reshape(F_DEV, D),
        expert_down,
    ).astype(bf16)


def solution(mesh):
    return jax.shard_map(
        on_device,
        mesh=mesh,
        in_specs=(
            P("ep", "tp"),
            P(),
            P("ep", "tp"),
            P("ep", "tp"),
            P("tp", "ep"),
            P("tp", "ep", None, None),
            P("tp", "ep", None, None),
            P("ep", None, "tp"),
            P("ep", None),
            P("ep", None),
        ),
        out_specs=P("ep", "tp"),
        check_vma=False,
    )
```

```python
import jax
import jax.numpy as jnp
from jax import lax
from jax.experimental import pallas as pl
from jax.experimental.pallas import tpu as pltpu
from jax.sharding import PartitionSpec as P

MESH = pl.DeviceIdType.MESH
EXP_DEV = 2
TOK_DEV = 384
CAP = 384
NZ, NY, NX = 8, 8, 4
N_TP, N_EP = 16, 32
SLOT, ROOM = 24, 32
F_DEV, F = 176, 1408
D, W = 2048, 128
norm_eps = 1e-06
bf16, f32, i32 = jnp.bfloat16, jnp.float32, jnp.int32


def rows_of(ref):
    count = ref.dtype.itemsize
    for n in ref.shape:
        count *= n
    return count // (2 * W)


class Link:
    def __init__(self, sems, gauge, groups):
        self.sems, self.gauge, self.groups = sems, gauge, groups
        self.keys, self.sent = {}, {}

    def _copy(self, src, dst, key, device, group):
        return pltpu.make_async_remote_copy(
            src_ref=src,
            dst_ref=dst,
            send_sem=self.sems.at[self.groups.index(group)],
            recv_sem=self.sems.at[self._at(key)],
            device_id=device,
            device_id_type=MESH,
        )

    def _at(self, key):
        if key in self.groups:
            return len(self.groups) + self.groups.index(key)
        return 2 * len(self.groups) + self.keys.setdefault(key, len(self.keys))

    def _all(self, index, rows):
        part = self.gauge.at[pl.ds(0, rows)]
        pltpu.make_async_copy(part, part, self.sems.at[index]).wait()

    def send(self, src, dst, key, device, group, core=None):
        self._copy(src, dst, key, device, group).start()
        held = self.sent.setdefault((group, core), [])
        held.append(rows_of(src))

    def arrive(self, dst, key, device, group):
        self._copy(dst, dst, key, device, group).wait_recv()

    def arrive_all(self, key, rows):
        self._all(self._at(key), rows)

    def finish(self):
        for (group, core), rows in self.sent.items():
            at, total = self.groups.index(group), sum(rows)
            if core is None:
                self._all(at, total)
            else:
                on_core(core)(lambda at=at, total=total: self._all(at, total))


def on_core(core):
    return pl.when(lax.rem(lax.axis_index("tp"), 2) == core)


def places():
    tp, ep = lax.axis_index("tp"), lax.axis_index("ep")
    return tp // 2, lax.rem(tp, 2), ep // NX, lax.rem(ep, NX)


def around(position, step, count):
    return lax.rem(position + step + count, count)


def z_device(z, core):
    return {"tp": z * 2 + core}


OFFSETS = sorted(
    [(a, b) for a in range(-3, 5) for b in range(-1, 3) if (a, b) != (0, 0)],
    key=lambda o: (o[1] % 4, o[0] % 8),
)


def greet():
    barrier = pltpu.get_barrier_semaphore()
    z, core, y, x = places()
    devices = [{"ep": around(y, a, NY) * NX + around(x, b, NX)} for a, b in OFFSETS]
    devices += [z_device(around(z, 1, NZ), core), z_device(around(z, -1, NZ), core)]
    devices += [z_device(z, 1 - core)]
    for device in devices:
        pl.semaphore_signal(barrier, inc=1, device_id=device, device_id_type=MESH)
    return len(devices)


class Exchange:
    def __init__(self, src, dst, src_all, dst_all, sems):
        self.src, self.dst, self.src_all, self.dst_all, self.sems = src, dst, src_all, dst_all, sems

    def start(self):
        _, _, y, x = places()
        own = y * NX + x
        for a, b in OFFSETS:
            peer = around(y, a, NY) * NX + around(x, b, NX)
            pltpu.make_async_remote_copy(
                src_ref=self.src(peer),
                dst_ref=self.dst(own),
                send_sem=self.sems.at[0],
                recv_sem=self.sems.at[1],
                device_id={"ep": peer},
                device_id_type=MESH,
            ).start()
        self.dst(own)[...] = self.src(own)[...]

    def arrive(self):
        part = self.dst_all
        pltpu.make_async_copy(part, part, self.sems.at[1]).wait()

    def finish(self):
        part = self.src_all
        pltpu.make_async_copy(part, part, self.sems.at[0]).wait()


def reach(direction, flipped):
    return 4 if (direction > 0) != bool(flipped) else 3


def ring_gather(pieces, link):
    def place():
        return lax.axis_index("tp") // 2

    def beside(d):
        return z_device(around(place(), d, NZ), 1)

    def mate(core):
        return z_device(place(), core)

    def ring(src, at, d, k, h, c):
        link.send(src, at, (d, k, h, c), beside(d), "ring", 1)

    def hand(block):
        link.send(block, block, "hand", mate(0), "hand", 1)
        handed.append(rows_of(block))

    handed = []
    numbered = list(enumerate(pieces))
    order = [(c, h, (flip + c) % 2, at) for c in (1, 0) for h, (flip, src, at) in numbered]
    whole = sum(rows_of(src) for flip, src, at in pieces)

    @on_core(1)
    def _():
        for h, (flip, src, at) in numbered:
            for d in (1, -1):
                ring(src, at(place() * 2 + 1), d, 1, h, 1)
        for flip, src, at in pieces:
            link.send(src, at(place() * 2 + 1), "hand", mate(0), "hand", 1)
            handed.append(rows_of(src))

    @on_core(0)
    def _():
        for flip, src, at in pieces:
            link.send(src, at(place() * 2), "join", mate(1), "join", 0)

    for flip, src, at in pieces:
        at(lax.axis_index("tp"))[...] = src[...]

    @on_core(1)
    def _():
        link.arrive_all("join", whole)
        for h, (flip, src, at) in numbered:
            for d in (1, -1):
                ring(at(place() * 2), at(place() * 2), d, 1, h, 0)

    yield
    for k in range(1, 5):

        @on_core(1)
        def _(k=k):
            for c, h, flip, at in order:
                for d in (1, -1):
                    most = reach(d, flip)
                    if k > most:
                        continue
                    block = at(around(place(), -d * k, NZ) * 2 + c)
                    link.arrive(block, (d, k, h, c), mate(0), "ring")
                    if k < most:
                        ring(block, block, d, k + 1, h, c)
                    hand(block)

        yield

    @on_core(0)
    def _():
        link.arrive_all("hand", sum(handed))

    yield


def plane_gather(src, dst, link, y_first):
    na, nb = (NY, NX) if y_first else (NX, NY)

    def at(da=0, db=0):
        _, _, y, x = places()
        if y_first:
            return around(y, da, NY) * NX + around(x, db, NX)
        return around(y, db, NY) * NX + around(x, da, NX)

    def mate(core):
        return z_device(places()[0], core)

    def ring(block, key, da, db):
        link.send(block, block, key, {"ep": at(da, db)}, "ring", 0)

    def hand(block):
        link.send(block.at[1], block.at[1], "hand", mate(1), "hand", 0)
        handed.append(rows_of(src))

    handed = []

    @on_core(1)
    def _():
        link.send(src, dst.at[at(), 1], "join", mate(0), "join", 1)

    dst[at(), lax.rem(lax.axis_index("tp"), 2)] = src[...]
    yield

    @on_core(0)
    def _():
        link.arrive_all("join", rows_of(src))
        block = dst.at[at()]
        for d in (1, -1):
            ring(block, ("a", d, 1), d, 0)
        for s in (1, -1):
            ring(block, ("b", s, 1, 0), 0, s)

    yield
    tags = [(0, 0)]
    for k in range(1, na // 2 + 1):
        for d in (1, -1):
            most = na // 2 if d > 0 else na // 2 - 1
            if k > most:
                continue

            @on_core(0)
            def _(d=d, k=k):
                block = dst.at[at(-d * k, 0)]
                link.arrive(block, ("a", d, k), {"ep": at()}, "ring")
                if k < most:
                    ring(block, ("a", d, k + 1), d, 0)
                for s in (1, -1):
                    ring(block, ("b", s, 1, len(tags)), 0, s)
                hand(block)

            tags.append((d, k))
            yield
    for j in range(1, nb // 2 + 1):
        for n, (d, k) in enumerate(tags):
            for s in (1, -1):
                most = nb // 2 if (s > 0) == (n % 2 == 0) else nb // 2 - 1
                if j > most:
                    continue

                @on_core(0)
                def _(d=d, k=k, s=s, j=j, n=n):
                    block = dst.at[at(-d * k, -s * j)]
                    link.arrive(block, ("b", s, j, n), {"ep": at()}, "ring")
                    if j < most:
                        ring(block, ("b", s, j + 1, n), 0, s)
                    hand(block)

                yield

    @on_core(1)
    def _():
        link.arrive_all("hand", sum(handed))

    yield


def go(job, steps=1000):
    for _ in range(steps):
        if next(job, "end") == "end":
            return


def one_hot(condition):
    return jnp.where(condition, 1.0, 0.0).astype(bf16)


def silu(v):
    return v / (1.0 + jnp.exp(-v))


def dims(a, b):
    return (((a,), (b,)), ((), ()))


def normalise(blocks, gain_ref, out_ref):
    for r in range(0, TOK_DEV, W):
        rows = pl.ds(r, W)
        squares = jnp.zeros((W, W), f32)
        for t in range(N_TP):
            wide = blocks(t)[rows, :].astype(f32)
            squares = squares + wide * wide
        inv = lax.rsqrt(jnp.sum(squares, axis=1, keepdims=True) * (1.0 / D) + norm_eps)
        for t in range(N_TP):
            lanes = slice(t * W, (t + 1) * W)
            wide = blocks(t)[rows, :].astype(f32)
            out_ref[rows, lanes] = (wide * inv * gain_ref[:, lanes]).astype(bf16)


def layer_kernel(
    chosen_hbm, sg_hbm, su_hbm, sd_hbm, tok_hbm, gain_hbm, gates_hbm, eg_hbm, eu_hbm, ed_hbm,
    mixed_ref,
    chosen_ref, sg_ref, su_ref, sd_ref, tok_ref, gain_ref, gates_ref,
    req_ref, gu_ref, dn_ref, wanted, asked, one_t, join, spread, out, came, tok_all, own, rows_all, wg, wd, hid, hid_all, back, returned,
    part, pair, got, made, eg, eu, ed, ed_t, normed, taken,
    load_sem, ask_sem, go_a, go_b, back_a, back_b,
    tok_sems, xa_sems, xb_sems, gu_sems, dn_sems, hid_sems, sum_sems,
):
    count = greet()
    z, core, _, _ = places()
    other = z_device(z, 1 - core)
    loads = [
        pltpu.make_async_copy(s, d, load_sem.at[i])
        for i, (s, d) in enumerate(
            (
                (chosen_hbm, chosen_ref),
                (sg_hbm, sg_ref),
                (su_hbm, su_ref),
                (sd_hbm, sd_ref),
                (tok_hbm, tok_ref),
                (gain_hbm, gain_ref),
                (gates_hbm, gates_ref),
                (eg_hbm, eg),
                (eu_hbm, eu),
                (ed_hbm, ed),
            )
        )
    ]
    for load in loads:
        load.start()
    loads[0].wait()
    slot_rows = []
    lane = lax.broadcasted_iota(i32, (CAP, W), 1)
    for e in range(EXP_DEV):
        ids = chosen_ref[e : e + 1, :]
        sources = owner_of(ids)
        ids_down = jnp.broadcast_to(ids, (W, CAP)).T
        sources_down = owner_of(ids_down)
        before = jnp.sum(
            jnp.where(jnp.concatenate([sources_down] * 3, axis=1) < sources, 1, 0), axis=0, keepdims=True
        )
        slots = sources * ROOM + lax.broadcasted_iota(i32, (1, CAP), 1) - before
        slot_rows.append(slots)
        slots_down = jnp.broadcast_to(slots, (W, CAP)).T
        local = ids_down - sources_down * TOK_DEV
        for b in range(N_EP * ROOM // W):
            match = slots_down == lane + b * W
            join[e, :, b * W : (b + 1) * W] = one_hot(match)
            wanted[e, b : b + 1] = jnp.max(jnp.where(match, local, -1), axis=0, keepdims=True)
    side = lax.rem(lax.axis_index("ep"), 2)
    lane = lax.broadcasted_iota(i32, (NY, W), 1)
    for i in range(NX):
        a, b = (pltpu.roll(wanted[e], (e - i) % NX * ROOM, 1) for e in range(EXP_DEV))
        both = jnp.where(lane < ROOM, a, jnp.where(lane < 2 * ROOM, b, -1))
        both = jnp.where(side == 0, both, pltpu.roll(both, W // 2, 1))
        for j in range(NY):
            req_ref[j * NX + i] = both[j : j + 1]
    came[...] = jnp.zeros_like(came)
    loads[4].wait()
    pl.semaphore_wait(pltpu.get_barrier_semaphore(), count)

    half = TOK_DEV // 2
    cuts = [pl.ds(0, half), pl.ds(half, half)]
    first = pl.ds(0, SLOT)
    some = pl.ds(0, N_EP - 1)

    half = TOK_DEV // 2
    cuts = [pl.ds(0, half), pl.ds(half, half)]
    first = pl.ds(0, SLOT)
    some = pl.ds(0, N_EP - 1)
    ask = Exchange(
        lambda p: req_ref.at[p], lambda p: asked.at[p], req_ref.at[some], asked.at[some], ask_sem
    )
    ask.start()
    kinds = ["ring", "hand", "join"]
    tok_link = Link(tok_sems, rows_all, kinds)
    tok_ring = ring_gather(
        [(0, tok_ref, lambda t: tok_all.at[t])], tok_link
    )
    go(tok_ring, 1)
    for load in loads[1:4]:
        load.wait()
    returned[...] = jnp.zeros_like(returned)
    gu_ref[:, :W] = sg_ref[:, :W]
    gu_ref[:, W : 2 * W] = su_ref[:, :W]
    gu_ref[:, 2 * W :] = jnp.concatenate(
        [sg_ref[:, W:], su_ref[:, W:], jnp.zeros((64, 32), bf16)], axis=1
    )
    dn_ref[...] = jnp.concatenate([sd_ref[...], jnp.zeros((64, 80), bf16)], axis=1)
    gu_link, dn_link = Link(gu_sems, rows_all, kinds), Link(dn_sems, rows_all, kinds)
    gu_job = plane_gather(gu_ref, wg, gu_link, True)
    dn_job = plane_gather(dn_ref, wd, dn_link, False)
    go(gu_job, 1)
    go(dn_job, 1)
    for e in range(EXP_DEV):
        at = lax.broadcasted_iota(i32, (N_EP * ROOM, CAP), 0)
        spread[e] = one_hot(at == slot_rows[e])
    go(tok_ring, 1)

    ask.arrive()
    token = lax.broadcasted_iota(i32, (TOK_DEV, W), 0)
    for i in range(N_EP // 2):
        ids = jnp.maximum(asked[2 * i], asked[2 * i + 1])
        one_t[:, i * W : (i + 1) * W] = one_hot(token == ids)
    for i in range(4):
        lanes = slice(i * 512, (i + 1) * 512)
        picked = lax.dot_general(
            one_t[:, lanes], tok_ref[...], dims(0, 0), preferred_element_type=f32
        )
        out[i * 8 : (i + 1) * 8] = picked.astype(bf16).reshape(8, EXP_DEV, ROOM, W)
    dispatch = [
        Exchange(
            lambda p, e=e: out.at[p, e, first],
            lambda p, e=e: came.at[e, p, first],
            out.at[some, e, first],
            came.at[e, some, first],
            sem,
        )
        for e, sem in enumerate((go_a, go_b))
    ]
    for e in range(EXP_DEV):
        dispatch[e].start()
    for load in loads[5:]:
        load.wait()
    for e in range(EXP_DEV):
        ed_t[e] = ed[e].T
    go(tok_ring, 1)
    go(tok_ring, 1)

    x_links = [Link(xa_sems, rows_all, kinds), Link(xb_sems, rows_all, kinds)]
    x_rings = []

    def taken_rows(t, e):
        return pl.ds(pl.multiple_of((t * EXP_DEV + e) * CAP, CAP), CAP)

    for e in range(EXP_DEV):
        dispatch[e].arrive()
        own[e] = jnp.dot(
            join[e], came[e].reshape(N_EP * ROOM, W), preferred_element_type=f32
        ).astype(bf16)
        x_rings.append(
            ring_gather(
                [(e, own.at[e], lambda t, e=e: rows_all.at[taken_rows(t, e)])],
                x_links[e],
            )
        )
        go(x_rings[e], 1)
        if e == 0:
            go(tok_ring, 1)
    for k in range(13):
        go(gu_job, 1)
        go(dn_job, 1)
    for k in range(4):
        for e in range(EXP_DEV):
            go(x_rings[e], 1)
    for e in range(EXP_DEV):
        go(x_rings[e], 1)

    expert = z // (NZ // EXP_DEV)
    normalise(lambda t: rows_all.at[taken_rows(t, expert)], gain_ref, taken)
    gate_values = lax.dot_general(eg[...], taken[...], dims(1, 1), preferred_element_type=f32)
    up_values = lax.dot_general(eu[...], taken[...], dims(1, 1), preferred_element_type=f32)
    hid[...] = (silu(gate_values) * up_values).astype(bf16)
    hid_link = Link(hid_sems, rows_all, kinds)
    hid_ring = ring_gather(
        [
            (h, hid.at[c], lambda t, c=c: hid_all.at[t, c])
            for h, c in enumerate((pl.ds(0, 96), pl.ds(96, 80)))
        ],
        hid_link,
    )
    go(hid_ring, 1)

    for k in range(18):
        go(gu_job, 1)
        go(dn_job, 1)
    go(tok_ring)
    normalise(lambda t: tok_all.at[t], gain_ref, normed)
    go(hid_ring, 1)
    go(hid_ring, 1)
    go(gu_job)
    mine = pl.ds(core, 1)
    weights = wg[:, mine].reshape(D, 384)
    sums = jnp.dot(normed[...], weights, preferred_element_type=f32)
    low = silu(sums[:, :W]) * sums[:, W : 2 * W]
    high = silu(sums[:, 256:304]) * sums[:, 304:352]
    shared = jnp.concatenate([low, high, jnp.zeros((TOK_DEV, 80), f32)], axis=1).astype(bf16)
    go(hid_ring, 1)
    go(dn_job)
    link = Link(sum_sems, rows_all, ["pair", "ring"])
    for t in range(N_TP):
        weights = wd[2 * t : 2 * t + 2, mine].reshape(W, 256)
        block = lax.dot_general(shared, weights, dims(1, 1), preferred_element_type=f32)
        part[t] = block.astype(bf16)
        if t % 2:
            i = t // 2
            link.send(part.at[2 * i + 1 - core], pair.at[i], "pair", other, "pair")
    link.arrive_all("pair", NZ * TOK_DEV)

    way = {1: 0, -1: 1}

    def term(m, rows):
        at = around(z, m, NZ)
        return part[at * 2 + core, rows].astype(f32) + pair[at, rows].astype(f32)

    def sum_round(k):
        for h, rows in enumerate(cuts):
            for d in (1, -1):
                most = reach(d, h)
                if k > most:
                    continue
                total = term(d * (most + 1 - k), rows)
                if k > 1:
                    link.arrive(got.at[way[d], k - 1, rows], (d, k - 1, h), other, "ring")
                    total = total + got[way[d], k - 1, rows].astype(f32)
                made[way[d], k, rows] = total.astype(bf16)
                src, dst = made.at[way[d], k, rows], got.at[way[d], k, rows]
                beside = z_device(around(z, d, NZ), core)
                link.send(src, dst, (d, k, h), beside, "ring")

    sum_round(1)
    go(hid_ring, 1)
    go(hid_ring)

    give = []
    for e in range(EXP_DEV):
        full = hid_all[e * 8 : (e + 1) * 8].reshape(F, CAP)
        outputs = jnp.dot(ed_t[e], full, preferred_element_type=f32)
        weighted = (outputs * gates_ref[e : e + 1, :]).astype(bf16)
        slots = lax.dot_general(spread[e], weighted, dims(1, 1), preferred_element_type=f32)
        back[e] = slots.astype(bf16).reshape(N_EP, ROOM, W)
        give.append(
            Exchange(
                lambda p, e=e: back.at[e, p, first],
                lambda p, e=e: returned.at[p, e, first],
                back.at[e, some, first],
                returned.at[some, e, first],
                (back_a, back_b)[e],
            )
        )
        give[e].start()

    for k in range(2, 5):
        sum_round(k)
    for h, rows in enumerate(cuts):
        total = term(0, rows)
        for d in (1, -1):
            most = reach(d, h)
            link.arrive(got.at[way[d], most, rows], (d, most, h), other, "ring")
            total = total + got[way[d], most, rows].astype(f32)
        mixed_ref[rows, :] = total
    for e in range(EXP_DEV):
        give[e].arrive()
    mixed_ref[...] += jnp.dot(
        one_t[...], returned[...].reshape(N_EP * 2 * ROOM, W), preferred_element_type=f32
    )
    for one in (ask, *dispatch, *give):
        one.finish()
    for one in (tok_link, *x_links, gu_link, dn_link, hid_link, link):
        one.finish()


def owner_of(ids):
    return ((ids >> 7) * 171) >> 9


def on_device(
    tokens,
    norm_gain,
    shared_gate,
    shared_up,
    shared_down,
    expert_gate,
    expert_up,
    expert_down,
    chosen,
    gates,
):
    vmem = pl.BlockSpec(memory_space=pltpu.VMEM)
    hbm = pl.BlockSpec(memory_space=pltpu.HBM)
    pool = lambda *shape, dtype=bf16: pltpu.VMEM(shape, dtype)
    dma = lambda n: pltpu.SemaphoreType.DMA((n,))
    return pl.pallas_call(
        layer_kernel,
        name="layer",
        out_shape=jax.ShapeDtypeStruct((TOK_DEV, W), f32),
        in_specs=[hbm] * 10,
        out_specs=vmem,
        scratch_shapes=[
            pool(EXP_DEV, CAP, dtype=i32),
            pool(64, F_DEV),
            pool(64, F_DEV),
            pool(64, F_DEV),
            pool(TOK_DEV, W),
            pool(1, D, dtype=f32),
            pool(EXP_DEV, CAP, dtype=f32),
            pool(N_EP, 1, W, dtype=i32),
            pool(64, 384),
            pool(64, 256),
            pool(EXP_DEV, NY, W, dtype=i32),
            pool(N_EP, 1, W, dtype=i32),
            pool(TOK_DEV, N_EP * 2 * ROOM),
            pool(EXP_DEV, CAP, N_EP * ROOM),
            pool(EXP_DEV, N_EP * ROOM, CAP),
            pool(N_EP, EXP_DEV, ROOM, W),
            pool(EXP_DEV, N_EP, ROOM, W),
            pool(N_TP, TOK_DEV, W),
            pool(EXP_DEV, CAP, W),
            pool(N_TP * EXP_DEV * CAP, W),
            pool(N_EP, 2, 64, 384),
            pool(N_EP, 2, 64, 256),
            pool(F_DEV, CAP),
            pool(N_TP, F_DEV, CAP),
            pool(EXP_DEV, N_EP, ROOM, W),
            pool(N_EP, EXP_DEV, ROOM, W),
            pool(N_TP, TOK_DEV, W),
            pool(NZ, TOK_DEV, W),
            pool(2, 5, TOK_DEV, W),
            pool(2, 5, TOK_DEV, W),
            pool(F_DEV, D),
            pool(F_DEV, D),
            pool(EXP_DEV, F, W),
            pool(EXP_DEV, W, F),
            pool(TOK_DEV, D),
            pool(CAP, D),
            dma(10),
            *[dma(2)] * 5,
            *[dma(20)] * 3,
            *[dma(37)] * 2,
            dma(34),
            dma(18),
        ],
        compiler_params=pltpu.CompilerParams(
            collective_id=0, has_side_effects=True, vmem_limit_bytes=56 * 1024 * 1024
        ),
    )(
        chosen,
        shared_gate,
        shared_up,
        shared_down.T,
        tokens,
        norm_gain.reshape(1, D),
        gates,
        expert_gate.reshape(F_DEV, D),
        expert_up.reshape(F_DEV, D),
        expert_down,
    ).astype(bf16)


def solution(mesh):
    return jax.shard_map(
        on_device,
        mesh=mesh,
        in_specs=(
            P("ep", "tp"),
            P(),
            P("ep", "tp"),
            P("ep", "tp"),
            P("tp", "ep"),
            P("tp", "ep", None, None),
            P("tp", "ep", None, None),
            P("ep", None, "tp"),
            P("ep", None),
            P("ep", None),
        ),
        out_specs=P("ep", "tp"),
        check_vma=False,
    )
```

```python
import jax
import jax.numpy as jnp
from jax import lax
from jax.experimental import pallas as pl
from jax.experimental.pallas import tpu as pltpu
from jax.sharding import PartitionSpec as P

MESH = pl.DeviceIdType.MESH
EXP_DEV = 2
TOK_DEV = 384
CAP = 384
NZ, NY, NX = 8, 8, 4
N_TP, N_EP = 16, 32
SLOT, ROOM = 24, 32
F_DEV, F = 176, 1408
D, W = 2048, 128
norm_eps = 1e-06
bf16, f32, i32 = jnp.bfloat16, jnp.float32, jnp.int32


def rows_of(ref):
    count = ref.dtype.itemsize
    for n in ref.shape:
        count *= n
    return count // (2 * W)


class Link:
    def __init__(self, sems, gauge, groups):
        self.sems, self.gauge, self.groups = sems, gauge, groups
        self.keys, self.sent = {}, {}

    def _copy(self, src, dst, key, device, group):
        return pltpu.make_async_remote_copy(
            src_ref=src,
            dst_ref=dst,
            send_sem=self.sems.at[self.groups.index(group)],
            recv_sem=self.sems.at[self._at(key)],
            device_id=device,
            device_id_type=MESH,
        )

    def _at(self, key):
        if key in self.groups:
            return len(self.groups) + self.groups.index(key)
        return 2 * len(self.groups) + self.keys.setdefault(key, len(self.keys))

    def _all(self, index, rows):
        part = self.gauge.at[pl.ds(0, rows)]
        pltpu.make_async_copy(part, part, self.sems.at[index]).wait()

    def send(self, src, dst, key, device, group, core=None):
        self._copy(src, dst, key, device, group).start()
        held = self.sent.setdefault((group, core), [])
        held.append(rows_of(src))

    def arrive(self, dst, key, device, group):
        self._copy(dst, dst, key, device, group).wait_recv()

    def arrive_all(self, key, rows):
        self._all(self._at(key), rows)

    def finish(self):
        for (group, core), rows in self.sent.items():
            at, total = self.groups.index(group), sum(rows)
            if core is None:
                self._all(at, total)
            else:
                on_core(core)(lambda at=at, total=total: self._all(at, total))


def on_core(core):
    return pl.when(lax.rem(lax.axis_index("tp"), 2) == core)


def places():
    tp, ep = lax.axis_index("tp"), lax.axis_index("ep")
    return tp // 2, lax.rem(tp, 2), ep // NX, lax.rem(ep, NX)


def around(position, step, count):
    return lax.rem(position + step + count, count)


def z_device(z, core):
    return {"tp": z * 2 + core}


OFFSETS = sorted(
    [(a, b) for a in range(-3, 5) for b in range(-1, 3) if (a, b) != (0, 0)],
    key=lambda o: (o[1] % 4, o[0] % 8),
)


def greet():
    barrier = pltpu.get_barrier_semaphore()
    z, core, y, x = places()
    devices = [{"ep": around(y, a, NY) * NX + around(x, b, NX)} for a, b in OFFSETS]
    devices += [z_device(around(z, 1, NZ), core), z_device(around(z, -1, NZ), core)]
    devices += [z_device(z, 1 - core)]
    for device in devices:
        pl.semaphore_signal(barrier, inc=1, device_id=device, device_id_type=MESH)
    return len(devices)


class Exchange:
    def __init__(self, src, dst, src_all, dst_all, sems):
        self.src, self.dst, self.src_all, self.dst_all, self.sems = src, dst, src_all, dst_all, sems

    def start(self):
        _, _, y, x = places()
        own = y * NX + x
        for a, b in OFFSETS:
            peer = around(y, a, NY) * NX + around(x, b, NX)
            pltpu.make_async_remote_copy(
                src_ref=self.src(peer),
                dst_ref=self.dst(own),
                send_sem=self.sems.at[0],
                recv_sem=self.sems.at[1],
                device_id={"ep": peer},
                device_id_type=MESH,
            ).start()
        self.dst(own)[...] = self.src(own)[...]

    def arrive(self):
        part = self.dst_all
        pltpu.make_async_copy(part, part, self.sems.at[1]).wait()

    def finish(self):
        part = self.src_all
        pltpu.make_async_copy(part, part, self.sems.at[0]).wait()


def reach(direction, flipped):
    return 4 if (direction > 0) != bool(flipped) else 3


def ring_gather(pieces, link):
    def place():
        return lax.axis_index("tp") // 2

    def beside(d):
        return z_device(around(place(), d, NZ), 1)

    def mate(core):
        return z_device(place(), core)

    def ring(src, at, d, k, h, c):
        link.send(src, at, (d, k, h, c), beside(d), "ring", 1)

    def hand(block):
        link.send(block, block, "hand", mate(0), "hand", 1)
        handed.append(rows_of(block))

    handed = []
    numbered = list(enumerate(pieces))
    order = [(c, h, (flip + c) % 2, at) for c in (1, 0) for h, (flip, src, at) in numbered]
    whole = sum(rows_of(src) for flip, src, at in pieces)

    @on_core(1)
    def _():
        for h, (flip, src, at) in numbered:
            for d in (1, -1):
                ring(src, at(place() * 2 + 1), d, 1, h, 1)
        for flip, src, at in pieces:
            link.send(src, at(place() * 2 + 1), "hand", mate(0), "hand", 1)
            handed.append(rows_of(src))

    @on_core(0)
    def _():
        for flip, src, at in pieces:
            link.send(src, at(place() * 2), "join", mate(1), "join", 0)

    for flip, src, at in pieces:
        at(lax.axis_index("tp"))[...] = src[...]

    @on_core(1)
    def _():
        link.arrive_all("join", whole)
        for h, (flip, src, at) in numbered:
            for d in (1, -1):
                ring(at(place() * 2), at(place() * 2), d, 1, h, 0)

    yield
    for k in range(1, 5):

        for c, h, flip, at in order:

            @on_core(1)
            def _(k=k, c=c, h=h, flip=flip, at=at):
                for d in (1, -1):
                    most = reach(d, flip)
                    if k > most:
                        continue
                    block = at(around(place(), -d * k, NZ) * 2 + c)
                    link.arrive(block, (d, k, h, c), mate(0), "ring")
                    if k < most:
                        ring(block, block, d, k + 1, h, c)
                    hand(block)

            yield

    @on_core(0)
    def _():
        link.arrive_all("hand", sum(handed))

    yield


def plane_gather(src, dst, link, y_first):
    na, nb = (NY, NX) if y_first else (NX, NY)

    def at(da=0, db=0):
        _, _, y, x = places()
        if y_first:
            return around(y, da, NY) * NX + around(x, db, NX)
        return around(y, db, NY) * NX + around(x, da, NX)

    def mate(core):
        return z_device(places()[0], core)

    def ring(block, key, da, db):
        link.send(block, block, key, {"ep": at(da, db)}, "ring", 0)

    def hand(block):
        link.send(block.at[1], block.at[1], "hand", mate(1), "hand", 0)
        handed.append(rows_of(src))

    handed = []

    @on_core(1)
    def _():
        link.send(src, dst.at[at(), 1], "join", mate(0), "join", 1)

    dst[at(), lax.rem(lax.axis_index("tp"), 2)] = src[...]
    yield

    @on_core(0)
    def _():
        link.arrive_all("join", rows_of(src))
        block = dst.at[at()]
        for d in (1, -1):
            ring(block, ("a", d, 1), d, 0)
        for s in (1, -1):
            ring(block, ("b", s, 1, 0), 0, s)

    yield
    def most(d, n, length):
        return length // 2 if (d > 0) == (n % 2 == 0) else length // 2 - 1

    tags = [(0, 0)] + [(d, k) for k in range(1, na // 2 + 1) for d in (1, -1) if k <= most(d, 0, na)]
    for wave in range(1, na // 2 + nb // 2 + 1):

        @on_core(0)
        def _(wave=wave):
            for n, (d, k) in enumerate(tags):
                if k == wave:
                    block = dst.at[at(-d * k, 0)]
                    link.arrive(block, ("a", d, k), {"ep": at()}, "ring")
                    if k < most(d, 0, na):
                        ring(block, ("a", d, k + 1), d, 0)
                    for s in (1, -1):
                        ring(block, ("b", s, 1, n), 0, s)
                    hand(block)
            for n, (d, k) in enumerate(tags):
                j = wave - k
                for s in (1, -1):
                    if not 1 <= j <= most(s, n, nb):
                        continue
                    block = dst.at[at(-d * k, -s * j)]
                    link.arrive(block, ("b", s, j, n), {"ep": at()}, "ring")
                    if j < most(s, n, nb):
                        ring(block, ("b", s, j + 1, n), 0, s)
                    hand(block)

        yield

    @on_core(1)
    def _():
        link.arrive_all("hand", sum(handed))

    yield


def go(job, steps=1000):
    for _ in range(steps):
        if next(job, "end") == "end":
            return


def one_hot(condition):
    return jnp.where(condition, 1.0, 0.0).astype(bf16)


def silu(v):
    return v / (1.0 + jnp.exp(-v))


def dims(a, b):
    return (((a,), (b,)), ((), ()))


def normalise(blocks, gain_ref, out_ref):
    for r in range(0, TOK_DEV, W):
        rows = pl.ds(r, W)
        squares = jnp.zeros((W, W), f32)
        for t in range(N_TP):
            wide = blocks(t)[rows, :].astype(f32)
            squares = squares + wide * wide
        inv = lax.rsqrt(jnp.sum(squares, axis=1, keepdims=True) * (1.0 / D) + norm_eps)
        for t in range(N_TP):
            lanes = slice(t * W, (t + 1) * W)
            wide = blocks(t)[rows, :].astype(f32)
            out_ref[rows, lanes] = (wide * inv * gain_ref[:, lanes]).astype(bf16)


def layer_kernel(
    chosen_hbm, sg_hbm, su_hbm, sd_hbm, tok_hbm, gain_hbm, gates_hbm, eg_hbm, eu_hbm, ed_hbm,
    mixed_ref,
    chosen_ref, sg_ref, su_ref, sd_ref, tok_ref, gain_ref, gates_ref,
    req_ref, gu_ref, dn_ref, wanted, asked, one_t, join, spread, out, came, tok_all, own, rows_all, wg, wd, hid, hid_all, back, returned,
    part, pair, got, made, eg, eu, ed, ed_t, normed, taken, shared,
    load_sem, ask_sem, go_a, go_b, back_a, back_b,
    turn_sem, tok_sems, xa_sems, xb_sems, gu_sems, dn_sems, hid_sems, sum_sems,
):
    z, core, _, _ = places()
    other = z_device(z, 1 - core)
    loads = [
        pltpu.make_async_copy(s, d, load_sem.at[i])
        for i, (s, d) in enumerate(
            (
                (chosen_hbm, chosen_ref),
                (sg_hbm, sg_ref),
                (su_hbm, su_ref),
                (sd_hbm, sd_ref),
                (tok_hbm, tok_ref),
                (gain_hbm, gain_ref),
                (gates_hbm, gates_ref),
                (eg_hbm, eg),
                (eu_hbm, eu),
                (ed_hbm, ed),
            )
        )
    ]
    for load in loads:
        load.start()
    count = greet()
    loads[0].wait()
    slot_rows = []
    lane = lax.broadcasted_iota(i32, (CAP, W), 1)
    for e in range(EXP_DEV):
        ids = chosen_ref[e : e + 1, :]
        sources = owner_of(ids)
        ids_down = jnp.broadcast_to(ids, (W, CAP)).T
        sources_down = owner_of(ids_down)
        before = jnp.sum(
            jnp.where(jnp.concatenate([sources_down] * 3, axis=1) < sources, 1, 0), axis=0, keepdims=True
        )
        slots = sources * ROOM + lax.broadcasted_iota(i32, (1, CAP), 1) - before
        slot_rows.append(slots)
        slots_down = jnp.broadcast_to(slots, (W, CAP)).T
        local = ids_down - sources_down * TOK_DEV
        for b in range(N_EP * ROOM // W):
            match = slots_down == lane + b * W
            join[e, :, b * W : (b + 1) * W] = one_hot(match)
            wanted[e, b : b + 1] = jnp.max(jnp.where(match, local, -1), axis=0, keepdims=True)
    side = lax.rem(lax.axis_index("ep"), 2)
    lane = lax.broadcasted_iota(i32, (NY, W), 1)
    for i in range(NX):
        a, b = (pltpu.roll(wanted[e], (e - i) % NX * ROOM, 1) for e in range(EXP_DEV))
        both = jnp.where(lane < ROOM, a, jnp.where(lane < 2 * ROOM, b, -1))
        both = jnp.where(side == 0, both, pltpu.roll(both, W // 2, 1))
        for j in range(NY):
            req_ref[j * NX + i] = both[j : j + 1]
    came[...] = jnp.zeros_like(came)
    loads[4].wait()
    pl.semaphore_wait(pltpu.get_barrier_semaphore(), count)

    half = TOK_DEV // 2
    cuts = [pl.ds(0, half), pl.ds(half, half)]
    first = pl.ds(0, SLOT)
    some = pl.ds(0, N_EP - 1)

    half = TOK_DEV // 2
    cuts = [pl.ds(0, half), pl.ds(half, half)]
    first = pl.ds(0, SLOT)
    some = pl.ds(0, N_EP - 1)
    ask = Exchange(
        lambda p: req_ref.at[p], lambda p: asked.at[p], req_ref.at[some], asked.at[some], ask_sem
    )
    ask.start()
    kinds = ["ring", "hand", "join"]
    tok_link = Link(tok_sems, rows_all, kinds)
    tok_ring = ring_gather(
        [(0, tok_ref, lambda t: tok_all.at[t])], tok_link
    )
    go(tok_ring, 1)
    for load in loads[1:4]:
        load.wait()
    returned[...] = jnp.zeros_like(returned)
    gu_ref[:, :W] = sg_ref[:, :W]
    gu_ref[:, W : 2 * W] = su_ref[:, :W]
    gu_ref[:, 2 * W :] = jnp.concatenate(
        [sg_ref[:, W:], su_ref[:, W:], jnp.zeros((64, 32), bf16)], axis=1
    )
    dn_ref[...] = jnp.concatenate([sd_ref[...], jnp.zeros((64, 80), bf16)], axis=1)
    gu_link, dn_link = Link(gu_sems, rows_all, kinds), Link(dn_sems, rows_all, kinds)
    gu_job = plane_gather(gu_ref, wg, gu_link, True)
    dn_job = plane_gather(dn_ref, wd, dn_link, False)
    go(gu_job, 1)
    go(dn_job, 1)
    for e in range(EXP_DEV):
        at = lax.broadcasted_iota(i32, (N_EP * ROOM, CAP), 0)
        spread[e] = one_hot(at == slot_rows[e])
    go(gu_job, 1)
    go(dn_job, 1)
    go(tok_ring, 2)

    ask.arrive()
    token = lax.broadcasted_iota(i32, (TOK_DEV, W), 0)
    for i in range(N_EP // 2):
        ids = jnp.maximum(asked[2 * i], asked[2 * i + 1])
        one_t[:, i * W : (i + 1) * W] = one_hot(token == ids)
    for i in range(4):
        lanes = slice(i * 512, (i + 1) * 512)
        picked = lax.dot_general(
            one_t[:, lanes], tok_ref[...], dims(0, 0), preferred_element_type=f32
        )
        out[i * 8 : (i + 1) * 8] = picked.astype(bf16).reshape(8, EXP_DEV, ROOM, W)
    dispatch = [
        Exchange(
            lambda p, e=e: out.at[p, e, first],
            lambda p, e=e: came.at[e, p, first],
            out.at[some, e, first],
            came.at[e, some, first],
            sem,
        )
        for e, sem in enumerate((go_a, go_b))
    ]
    for e in range(EXP_DEV):
        dispatch[e].start()
    for load in loads[5:]:
        load.wait()
    for e in range(EXP_DEV):
        ed_t[e] = ed[e].T
    go(tok_ring, 2)
    go(tok_ring, 2)

    x_links = [Link(xa_sems, rows_all, kinds), Link(xb_sems, rows_all, kinds)]
    x_rings = []

    def taken_rows(t, e):
        return pl.ds(pl.multiple_of((t * EXP_DEV + e) * CAP, CAP), CAP)

    for e in range(EXP_DEV):
        dispatch[e].arrive()
        own[e] = jnp.dot(
            join[e], came[e].reshape(N_EP * ROOM, W), preferred_element_type=f32
        ).astype(bf16)
        x_rings.append(
            ring_gather(
                [(e, own.at[e], lambda t, e=e: rows_all.at[taken_rows(t, e)])],
                x_links[e],
            )
        )
        go(x_rings[e], 1)
        if e == 0:
            go(tok_ring, 2)
    for wave in range(4):
        go(gu_job, 1)
        go(dn_job, 1)
    for k in range(4):
        for e in range(EXP_DEV):
            go(x_rings[e], 2)
    for e in range(EXP_DEV):
        go(x_rings[e], 1)

    expert = z // (NZ // EXP_DEV)
    normalise(lambda t: rows_all.at[taken_rows(t, expert)], gain_ref, taken)
    gate_values = lax.dot_general(eg[...], taken[...], dims(1, 1), preferred_element_type=f32)
    up_values = lax.dot_general(eu[...], taken[...], dims(1, 1), preferred_element_type=f32)
    hid[...] = (silu(gate_values) * up_values).astype(bf16)
    hid_link = Link(hid_sems, rows_all, kinds)
    hid_ring = ring_gather(
        [
            (h, hid.at[c], lambda t, c=c: hid_all.at[t, c])
            for h, c in enumerate((pl.ds(0, 96), pl.ds(96, 80)))
        ],
        hid_link,
    )
    go(hid_ring, 1)

    go(tok_ring)
    normalise(lambda t: tok_all.at[t], gain_ref, normed)
    for wave in range(2):
        go(gu_job, 1)
        go(dn_job, 1)
    go(hid_ring, 4)
    go(gu_job)
    go(hid_ring, 1)
    mine = pl.ds(core, 1)
    weights = wg[:, mine].reshape(D, 384)
    for i in range(3):
        block = pl.ds(i * W, W)
        sums = jnp.dot(normed[block, :], weights, preferred_element_type=f32)
        low = silu(sums[:, :W]) * sums[:, W : 2 * W]
        high = silu(sums[:, 256:304]) * sums[:, 304:352]
        shared[block, :] = jnp.concatenate([low, high, jnp.zeros((W, 80), f32)], axis=1).astype(bf16)
        go(hid_ring, 1)
    go(dn_job)
    link = Link(sum_sems, rows_all, ["pair", "ring"])
    for t in range(N_TP):
        if t % 4 == 0:
            go(hid_ring, 1)
        weights = wd[2 * t : 2 * t + 2, mine].reshape(W, 256)
        block = lax.dot_general(shared[...], weights, dims(1, 1), preferred_element_type=f32)
        part[t] = block.astype(bf16)
        if t % 2:
            i = t // 2
            link.send(part.at[2 * i + 1 - core], pair.at[i], "pair", other, "pair")
    link.arrive_all("pair", NZ * TOK_DEV)

    way = {1: 0, -1: 1}

    def term(m, rows):
        at = around(z, m, NZ)
        return part[at * 2 + core, rows].astype(f32) + pair[at, rows].astype(f32)

    def sum_round(k):
        for h, rows in enumerate(cuts):
            for d in (1, -1):
                most = reach(d, h)
                if k > most:
                    continue
                total = term(d * (most + 1 - k), rows)
                if k > 1:
                    link.arrive(got.at[way[d], k - 1, rows], (d, k - 1, h), other, "ring")
                    total = total + got[way[d], k - 1, rows].astype(f32)
                made[way[d], k, rows] = total.astype(bf16)
                src, dst = made.at[way[d], k, rows], got.at[way[d], k, rows]
                beside = z_device(around(z, d, NZ), core)
                link.send(src, dst, (d, k, h), beside, "ring")


    @on_core(1)
    def _():
        pl.semaphore_signal(turn_sem, inc=1, device_id=other, device_id_type=MESH)

    @on_core(0)
    def _():
        pl.semaphore_wait(turn_sem, 1)

    sum_round(1)
    go(hid_ring, 4)
    go(hid_ring)

    give = []
    for e in range(EXP_DEV):
        full = hid_all[e * 8 : (e + 1) * 8].reshape(F, CAP)
        outputs = jnp.dot(ed_t[e], full, preferred_element_type=f32)
        weighted = (outputs * gates_ref[e : e + 1, :]).astype(bf16)
        slots = lax.dot_general(spread[e], weighted, dims(1, 1), preferred_element_type=f32)
        back[e] = slots.astype(bf16).reshape(N_EP, ROOM, W)
        give.append(
            Exchange(
                lambda p, e=e: back.at[e, p, first],
                lambda p, e=e: returned.at[p, e, first],
                back.at[e, some, first],
                returned.at[some, e, first],
                (back_a, back_b)[e],
            )
        )
        give[e].start()
        if e == 0:
            sum_round(2)

    for k in range(3, 5):
        sum_round(k)
    for h, rows in enumerate(cuts):
        total = term(0, rows)
        for d in (1, -1):
            most = reach(d, h)
            link.arrive(got.at[way[d], most, rows], (d, most, h), other, "ring")
            total = total + got[way[d], most, rows].astype(f32)
        mixed_ref[rows, :] = total
    for e in range(EXP_DEV):
        give[e].arrive()
    mixed_ref[...] += jnp.dot(
        one_t[...], returned[...].reshape(N_EP * 2 * ROOM, W), preferred_element_type=f32
    )
    for one in (ask, *dispatch, *give):
        one.finish()
    for one in (tok_link, *x_links, gu_link, dn_link, hid_link, link):
        one.finish()


def owner_of(ids):
    return ((ids >> 7) * 171) >> 9


def on_device(
    tokens,
    norm_gain,
    shared_gate,
    shared_up,
    shared_down,
    expert_gate,
    expert_up,
    expert_down,
    chosen,
    gates,
):
    vmem = pl.BlockSpec(memory_space=pltpu.VMEM)
    hbm = pl.BlockSpec(memory_space=pltpu.HBM)
    pool = lambda *shape, dtype=bf16: pltpu.VMEM(shape, dtype)
    dma = lambda n: pltpu.SemaphoreType.DMA((n,))
    return pl.pallas_call(
        layer_kernel,
        name="layer",
        out_shape=jax.ShapeDtypeStruct((TOK_DEV, W), f32),
        in_specs=[hbm] * 10,
        out_specs=vmem,
        scratch_shapes=[
            pool(EXP_DEV, CAP, dtype=i32),
            pool(64, F_DEV),
            pool(64, F_DEV),
            pool(64, F_DEV),
            pool(TOK_DEV, W),
            pool(1, D, dtype=f32),
            pool(EXP_DEV, CAP, dtype=f32),
            pool(N_EP, 1, W, dtype=i32),
            pool(64, 384),
            pool(64, 256),
            pool(EXP_DEV, NY, W, dtype=i32),
            pool(N_EP, 1, W, dtype=i32),
            pool(TOK_DEV, N_EP * 2 * ROOM),
            pool(EXP_DEV, CAP, N_EP * ROOM),
            pool(EXP_DEV, N_EP * ROOM, CAP),
            pool(N_EP, EXP_DEV, ROOM, W),
            pool(EXP_DEV, N_EP, ROOM, W),
            pool(N_TP, TOK_DEV, W),
            pool(EXP_DEV, CAP, W),
            pool(N_TP * EXP_DEV * CAP, W),
            pool(N_EP, 2, 64, 384),
            pool(N_EP, 2, 64, 256),
            pool(F_DEV, CAP),
            pool(N_TP, F_DEV, CAP),
            pool(EXP_DEV, N_EP, ROOM, W),
            pool(N_EP, EXP_DEV, ROOM, W),
            pool(N_TP, TOK_DEV, W),
            pool(NZ, TOK_DEV, W),
            pool(2, 5, TOK_DEV, W),
            pool(2, 5, TOK_DEV, W),
            pool(F_DEV, D),
            pool(F_DEV, D),
            pool(EXP_DEV, F, W),
            pool(EXP_DEV, W, F),
            pool(TOK_DEV, D),
            pool(CAP, D),
            pool(TOK_DEV, 256),
            dma(10),
            *[dma(2)] * 5,
            pltpu.SemaphoreType.REGULAR,
            *[dma(20)] * 3,
            *[dma(37)] * 2,
            dma(34),
            dma(18),
        ],
        compiler_params=pltpu.CompilerParams(
            collective_id=0, has_side_effects=True, vmem_limit_bytes=56 * 1024 * 1024
        ),
    )(
        chosen,
        shared_gate,
        shared_up,
        shared_down.T,
        tokens,
        norm_gain.reshape(1, D),
        gates,
        expert_gate.reshape(F_DEV, D),
        expert_up.reshape(F_DEV, D),
        expert_down,
    ).astype(bf16)


def solution(mesh):
    return jax.shard_map(
        on_device,
        mesh=mesh,
        in_specs=(
            P("ep", "tp"),
            P(),
            P("ep", "tp"),
            P("ep", "tp"),
            P("tp", "ep"),
            P("tp", "ep", None, None),
            P("tp", "ep", None, None),
            P("ep", None, "tp"),
            P("ep", None),
            P("ep", None),
        ),
        out_specs=P("ep", "tp"),
        check_vma=False,
    )
```

```python
import jax
import jax.numpy as jnp
from jax import lax
from jax.experimental import pallas as pl
from jax.experimental.pallas import tpu as pltpu
from jax.sharding import PartitionSpec as P

MESH = pl.DeviceIdType.MESH
EXP_DEV = 2
TOK_DEV = 384
CAP = 384
NZ, NY, NX = 8, 8, 4
N_TP, N_EP = 16, 32
SLOT, ROOM = 24, 32
F_DEV, F = 176, 1408
D, W = 2048, 128
norm_eps = 1e-06
bf16, f32, i32 = jnp.bfloat16, jnp.float32, jnp.int32


def rows_of(ref):
    count = ref.dtype.itemsize
    for n in ref.shape:
        count *= n
    return count // (2 * W)


class Link:
    def __init__(self, sems, gauge, groups):
        self.sems, self.gauge, self.groups = sems, gauge, groups
        self.keys, self.sent = {}, {}

    def _copy(self, src, dst, key, device, group):
        sent = self.groups.index(group) if group in self.groups else self._at(("sent", key))
        return pltpu.make_async_remote_copy(
            src_ref=src,
            dst_ref=dst,
            send_sem=self.sems.at[sent],
            recv_sem=self.sems.at[self._at(key)],
            device_id=device,
            device_id_type=MESH,
        )

    def _at(self, key):
        if key in self.groups:
            return len(self.groups) + self.groups.index(key)
        return 2 * len(self.groups) + self.keys.setdefault(key, len(self.keys))

    def _all(self, index, rows):
        part = self.gauge.at[pl.ds(0, rows)]
        pltpu.make_async_copy(part, part, self.sems.at[index]).wait()

    def send(self, src, dst, key, device, group, core=None, wanted=None):
        self._copy(src, dst, key, device, group).start()
        at = self.groups.index(group) if group in self.groups else self._at(("sent", key))
        self.sent.setdefault((at, core), [wanted, 0])[1] += rows_of(src)

    def arrive(self, dst, key, device, group):
        self._copy(dst, dst, key, device, group).wait_recv()

    def arrive_all(self, key, rows):
        self._all(self._at(key), rows)

    def finish(self):
        for (at, core), (wanted, rows) in self.sent.items():
            here = True if core is None else lax.rem(lax.axis_index("tp"), 2) == core
            if wanted is not None:
                here = jnp.logical_and(here, wanted())
            when(here)(lambda at=at, rows=rows: self._all(at, rows))


def when(condition):
    return (lambda f: f()) if condition is True else pl.when(condition)


def on_core(core):
    return pl.when(lax.rem(lax.axis_index("tp"), 2) == core)


def places():
    tp, ep = lax.axis_index("tp"), lax.axis_index("ep")
    return tp // 2, lax.rem(tp, 2), ep // NX, lax.rem(ep, NX)


def around(position, step, count):
    return lax.rem(position + step + count, count)


def z_device(z, core):
    return {"tp": z * 2 + core}


OFFSETS = sorted(
    [(a, b) for a in range(-3, 5) for b in range(-1, 3) if (a, b) != (0, 0)],
    key=lambda o: (o[1] % 4, o[0] % 8),
)


def greet():
    barrier = pltpu.get_barrier_semaphore()
    z, core, y, x = places()
    devices = [{"ep": around(y, a, NY) * NX + around(x, b, NX)} for a, b in OFFSETS]
    devices += [z_device(around(z, 1, NZ), core), z_device(around(z, -1, NZ), core)]
    devices += [z_device(z, 1 - core)]
    for device in devices:
        pl.semaphore_signal(barrier, inc=1, device_id=device, device_id_type=MESH)
    return len(devices)


class Exchange:
    def __init__(self, src, dst, src_all, dst_all, sems):
        self.src, self.dst, self.src_all, self.dst_all, self.sems = src, dst, src_all, dst_all, sems

    def start(self):
        _, _, y, x = places()
        own = y * NX + x
        for a, b in OFFSETS:
            peer = around(y, a, NY) * NX + around(x, b, NX)
            pltpu.make_async_remote_copy(
                src_ref=self.src(peer),
                dst_ref=self.dst(own),
                send_sem=self.sems.at[0],
                recv_sem=self.sems.at[1],
                device_id={"ep": peer},
                device_id_type=MESH,
            ).start()
        self.dst(own)[...] = self.src(own)[...]

    def arrive(self):
        part = self.dst_all
        pltpu.make_async_copy(part, part, self.sems.at[1]).wait()

    def finish(self):
        part = self.src_all
        pltpu.make_async_copy(part, part, self.sems.at[0]).wait()


def reach(direction, flipped):
    return 4 if (direction > 0) != bool(flipped) else 3


def ring_gather(pieces, link, taker=None):
    def place():
        return lax.axis_index("tp") // 2

    def beside(d):
        return z_device(around(place(), d, NZ), 1)

    def mate(core):
        return z_device(place(), core)

    def takes():
        return True if taker is None else place() // (NZ // EXP_DEV) == taker

    def goes(d, k, flip, back):
        if taker is None:
            return True
        half = NZ // EXP_DEV
        v = lax.rem(place() - d * back - half * taker + 2 * NZ, NZ)
        if d < 0:
            v = lax.rem(half - 1 - v + NZ, NZ)
        last = half - 1 if reach(d, flip) == half else half
        return jnp.logical_or(v < half - k, v > last)

    def ring(src, at, d, k, h, c, flip, back):
        key, group = (d, k, h, c), "ring" if taker is None else None
        wanted = None if taker is None else lambda: goes(d, k, flip, back)
        link.send(src, at, key, beside(d), group, 1, wanted)

    def hand(src, dst):
        link.send(src, dst, "hand", mate(0), "hand", 1, None if taker is None else takes)
        handed.append(rows_of(src))

    handed = []
    numbered = list(enumerate(pieces))
    order = [(c, h, (flip + c) % 2, at) for c in (1, 0) for h, (flip, src, at) in numbered]
    whole = sum(rows_of(src) for flip, src, at in pieces)

    @on_core(1)
    def _():
        for h, (flip, src, at) in numbered:
            for d in (1, -1):

                @when(goes(d, 1, (flip + 1) % 2, 0))
                def _(d=d, h=h, flip=flip, src=src, at=at):
                    ring(src, at(place() * 2 + 1), d, 1, h, 1, (flip + 1) % 2, 0)

        for flip, src, at in pieces:
            when(takes())(lambda src=src, at=at: hand(src, at(place() * 2 + 1)))

    @on_core(0)
    def _():
        for flip, src, at in pieces:
            link.send(src, at(place() * 2), "join", mate(1), "join", 0)

    for flip, src, at in pieces:
        at(lax.axis_index("tp"))[...] = src[...]

    @on_core(1)
    def _():
        link.arrive_all("join", whole)
        for h, (flip, src, at) in numbered:
            for d in (1, -1):

                @when(goes(d, 1, flip, 0))
                def _(d=d, h=h, flip=flip, at=at):
                    ring(at(place() * 2), at(place() * 2), d, 1, h, 0, flip, 0)

    yield
    for k in range(1, 5):
        for c, h, flip, at in order:

            def step(d, k=k, c=c, h=h, flip=flip, at=at):
                block = at(around(place(), -d * k, NZ) * 2 + c)
                link.arrive(block, (d, k, h, c), mate(0), "ring" if taker is None else None)
                if k < reach(d, flip):
                    when(goes(d, k + 1, flip, k))(lambda: ring(block, block, d, k + 1, h, c, flip, k))
                when(takes())(lambda: hand(block, block))

            @on_core(1)
            def _(k=k, flip=flip, step=step):
                for d in (1, -1):
                    if k <= reach(d, flip):
                        when(goes(d, k, flip, k))(lambda d=d: step(d))

            yield

    @on_core(0)
    def _():
        when(takes())(lambda: link.arrive_all("hand", sum(handed)))

    yield


def plane_gather(src, dst, link, y_first):
    na, nb = (NY, NX) if y_first else (NX, NY)

    def at(da=0, db=0):
        _, _, y, x = places()
        if y_first:
            return around(y, da, NY) * NX + around(x, db, NX)
        return around(y, db, NY) * NX + around(x, da, NX)

    def mate(core):
        return z_device(places()[0], core)

    def ring(block, key, da, db):
        link.send(block, block, key, {"ep": at(da, db)}, "ring", 0)

    def hand(block):
        link.send(block.at[1], block.at[1], "hand", mate(1), "hand", 0)
        handed.append(rows_of(src))

    handed = []

    @on_core(1)
    def _():
        link.send(src, dst.at[at(), 1], "join", mate(0), "join", 1)

    dst[at(), lax.rem(lax.axis_index("tp"), 2)] = src[...]
    yield

    @on_core(0)
    def _():
        link.arrive_all("join", rows_of(src))
        block = dst.at[at()]
        for d in (1, -1):
            ring(block, ("a", d, 1), d, 0)
        for s in (1, -1):
            ring(block, ("b", s, 1, 0), 0, s)

    yield
    def most(d, n, length):
        return length // 2 if (d > 0) == (n % 2 == 0) else length // 2 - 1

    tags = [(0, 0)] + [(d, k) for k in range(1, na // 2 + 1) for d in (1, -1) if k <= most(d, 0, na)]
    for wave in range(1, na // 2 + nb // 2 + 1):

        @on_core(0)
        def _(wave=wave):
            for n, (d, k) in enumerate(tags):
                if k == wave:
                    block = dst.at[at(-d * k, 0)]
                    link.arrive(block, ("a", d, k), {"ep": at()}, "ring")
                    if k < most(d, 0, na):
                        ring(block, ("a", d, k + 1), d, 0)
                    for s in (1, -1):
                        ring(block, ("b", s, 1, n), 0, s)
                    hand(block)
            for n, (d, k) in enumerate(tags):
                j = wave - k
                for s in (1, -1):
                    if not 1 <= j <= most(s, n, nb):
                        continue
                    block = dst.at[at(-d * k, -s * j)]
                    link.arrive(block, ("b", s, j, n), {"ep": at()}, "ring")
                    if j < most(s, n, nb):
                        ring(block, ("b", s, j + 1, n), 0, s)
                    hand(block)

        yield

    @on_core(1)
    def _():
        link.arrive_all("hand", sum(handed))

    yield


def go(job, steps=1000):
    for _ in range(steps):
        if next(job, "end") == "end":
            return


def one_hot(condition):
    return jnp.where(condition, 1.0, 0.0).astype(bf16)


def silu(v):
    return v / (1.0 + jnp.exp(-v))


def dims(a, b):
    return (((a,), (b,)), ((), ()))


def normalise(blocks, gain_ref, out_ref):
    for r in range(0, TOK_DEV, W):
        rows = pl.ds(r, W)
        squares = jnp.zeros((W, W), f32)
        for t in range(N_TP):
            wide = blocks(t)[rows, :].astype(f32)
            squares = squares + wide * wide
        inv = lax.rsqrt(jnp.sum(squares, axis=1, keepdims=True) * (1.0 / D) + norm_eps)
        for t in range(N_TP):
            lanes = slice(t * W, (t + 1) * W)
            wide = blocks(t)[rows, :].astype(f32)
            out_ref[rows, lanes] = (wide * inv * gain_ref[:, lanes]).astype(bf16)


def layer_kernel(
    chosen_hbm, sg_hbm, su_hbm, sd_hbm, tok_hbm, gain_hbm, gates_hbm, eg_hbm, eu_hbm, ed_hbm,
    mixed_ref,
    chosen_ref, sg_ref, su_ref, sd_ref, tok_ref, gain_ref, gates_ref,
    req_ref, gu_ref, dn_ref, wanted, asked, one_t, join, spread, out, came, tok_all, own, rows_all, wg, wd, hid, hid_all, back, returned,
    part, pair, got, made, eg, eu, ed, ed_t, normed, taken, shared,
    load_sem, ask_sem, go_a, go_b, back_a, back_b,
    turn_sem, tok_sems, xa_sems, xb_sems, gu_sems, dn_sems, hid_sems, sum_sems,
):
    z, core, _, _ = places()
    other = z_device(z, 1 - core)
    loads = [
        pltpu.make_async_copy(s, d, load_sem.at[i])
        for i, (s, d) in enumerate(
            (
                (chosen_hbm, chosen_ref),
                (sg_hbm, sg_ref),
                (su_hbm, su_ref),
                (sd_hbm, sd_ref),
                (tok_hbm, tok_ref),
                (gain_hbm, gain_ref),
                (gates_hbm, gates_ref),
                (eg_hbm, eg),
                (eu_hbm, eu),
                (ed_hbm, ed),
            )
        )
    ]
    for load in loads:
        load.start()
    count = greet()
    loads[0].wait()
    slot_rows = []
    lane = lax.broadcasted_iota(i32, (CAP, W), 1)
    for e in range(EXP_DEV):
        ids = chosen_ref[e : e + 1, :]
        sources = owner_of(ids)
        ids_down = jnp.broadcast_to(ids, (W, CAP)).T
        sources_down = owner_of(ids_down)
        before = jnp.sum(
            jnp.where(jnp.concatenate([sources_down] * 3, axis=1) < sources, 1, 0), axis=0, keepdims=True
        )
        slots = sources * ROOM + lax.broadcasted_iota(i32, (1, CAP), 1) - before
        slot_rows.append(slots)
        slots_down = jnp.broadcast_to(slots, (W, CAP)).T
        local = ids_down - sources_down * TOK_DEV
        for b in range(N_EP * ROOM // W):
            match = slots_down == lane + b * W
            join[e, :, b * W : (b + 1) * W] = one_hot(match)
            wanted[e, b : b + 1] = jnp.max(jnp.where(match, local, -1), axis=0, keepdims=True)
    side = lax.rem(lax.axis_index("ep"), 2)
    lane = lax.broadcasted_iota(i32, (NY, W), 1)
    for i in range(NX):
        a, b = (pltpu.roll(wanted[e], (e - i) % NX * ROOM, 1) for e in range(EXP_DEV))
        both = jnp.where(lane < ROOM, a, jnp.where(lane < 2 * ROOM, b, -1))
        both = jnp.where(side == 0, both, pltpu.roll(both, W // 2, 1))
        for j in range(NY):
            req_ref[j * NX + i] = both[j : j + 1]
    came[...] = jnp.zeros_like(came)
    loads[4].wait()
    pl.semaphore_wait(pltpu.get_barrier_semaphore(), count)

    half = TOK_DEV // 2
    cuts = [pl.ds(0, half), pl.ds(half, half)]
    first = pl.ds(0, SLOT)
    some = pl.ds(0, N_EP - 1)

    half = TOK_DEV // 2
    cuts = [pl.ds(0, half), pl.ds(half, half)]
    first = pl.ds(0, SLOT)
    some = pl.ds(0, N_EP - 1)
    ask = Exchange(
        lambda p: req_ref.at[p], lambda p: asked.at[p], req_ref.at[some], asked.at[some], ask_sem
    )
    ask.start()
    kinds = ["ring", "hand", "join"]
    tok_link = Link(tok_sems, rows_all, kinds)
    tok_ring = ring_gather(
        [(0, tok_ref, lambda t: tok_all.at[t])], tok_link
    )
    go(tok_ring, 1)
    for load in loads[1:4]:
        load.wait()
    returned[...] = jnp.zeros_like(returned)
    gu_ref[:, :W] = sg_ref[:, :W]
    gu_ref[:, W : 2 * W] = su_ref[:, :W]
    gu_ref[:, 2 * W :] = jnp.concatenate(
        [sg_ref[:, W:], su_ref[:, W:], jnp.zeros((64, 32), bf16)], axis=1
    )
    dn_ref[...] = jnp.concatenate([sd_ref[...], jnp.zeros((64, 80), bf16)], axis=1)
    gu_link, dn_link = Link(gu_sems, rows_all, kinds), Link(dn_sems, rows_all, kinds)
    gu_job = plane_gather(gu_ref, wg, gu_link, True)
    dn_job = plane_gather(dn_ref, wd, dn_link, False)
    go(gu_job, 1)
    go(dn_job, 1)
    for e in range(EXP_DEV):
        at = lax.broadcasted_iota(i32, (N_EP * ROOM, CAP), 0)
        spread[e] = one_hot(at == slot_rows[e])
    go(gu_job, 1)
    go(dn_job, 1)
    go(tok_ring, 2)

    ask.arrive()
    token = lax.broadcasted_iota(i32, (TOK_DEV, W), 0)
    for i in range(N_EP // 2):
        ids = jnp.maximum(asked[2 * i], asked[2 * i + 1])
        one_t[:, i * W : (i + 1) * W] = one_hot(token == ids)
    for i in range(4):
        lanes = slice(i * 512, (i + 1) * 512)
        picked = lax.dot_general(
            one_t[:, lanes], tok_ref[...], dims(0, 0), preferred_element_type=f32
        )
        out[i * 8 : (i + 1) * 8] = picked.astype(bf16).reshape(8, EXP_DEV, ROOM, W)
    dispatch = [
        Exchange(
            lambda p, e=e: out.at[p, e, first],
            lambda p, e=e: came.at[e, p, first],
            out.at[some, e, first],
            came.at[e, some, first],
            sem,
        )
        for e, sem in enumerate((go_a, go_b))
    ]
    for e in range(EXP_DEV):
        dispatch[e].start()
    for load in loads[5:]:
        load.wait()
    for e in range(EXP_DEV):
        ed_t[e] = ed[e].T
    go(tok_ring, 2)
    go(tok_ring, 2)

    x_links = [Link(xa_sems, rows_all, kinds), Link(xb_sems, rows_all, kinds)]
    x_rings = []

    def taken_rows(t, e):
        return pl.ds(pl.multiple_of((t * EXP_DEV + e) * CAP, CAP), CAP)

    for e in range(EXP_DEV):
        dispatch[e].arrive()
        own[e] = jnp.dot(
            join[e], came[e].reshape(N_EP * ROOM, W), preferred_element_type=f32
        ).astype(bf16)
        x_rings.append(
            ring_gather(
                [(e, own.at[e], lambda t, e=e: rows_all.at[taken_rows(t, e)])],
                x_links[e],
                e,
            )
        )
        go(x_rings[e], 1)
        if e == 0:
            go(tok_ring, 2)
            go(gu_job, 1)
            go(dn_job, 1)
    for wave in range(3):
        go(gu_job, 1)
        go(dn_job, 1)
    for k in range(4):
        for e in range(EXP_DEV):
            go(x_rings[e], 2)
    for e in range(EXP_DEV):
        go(x_rings[e], 1)

    expert = z // (NZ // EXP_DEV)
    normalise(lambda t: rows_all.at[taken_rows(t, expert)], gain_ref, taken)
    gate_values = lax.dot_general(eg[...], taken[...], dims(1, 1), preferred_element_type=f32)
    up_values = lax.dot_general(eu[...], taken[...], dims(1, 1), preferred_element_type=f32)
    hid[...] = (silu(gate_values) * up_values).astype(bf16)
    hid_link = Link(hid_sems, rows_all, kinds)
    hid_ring = ring_gather(
        [
            (h, hid.at[c], lambda t, c=c: hid_all.at[t, c])
            for h, c in enumerate((pl.ds(0, 96), pl.ds(96, 80)))
        ],
        hid_link,
    )
    go(hid_ring, 1)

    go(tok_ring)
    normalise(lambda t: tok_all.at[t], gain_ref, normed)
    for wave in range(2):
        go(gu_job, 1)
        go(dn_job, 1)
    go(hid_ring, 4)
    go(gu_job)
    go(hid_ring, 1)
    mine = pl.ds(core, 1)
    weights = wg[:, mine].reshape(D, 384)
    for i in range(3):
        block = pl.ds(i * W, W)
        sums = jnp.dot(normed[block, :], weights, preferred_element_type=f32)
        low = silu(sums[:, :W]) * sums[:, W : 2 * W]
        high = silu(sums[:, 256:304]) * sums[:, 304:352]
        shared[block, :] = jnp.concatenate([low, high, jnp.zeros((W, 80), f32)], axis=1).astype(bf16)
        go(hid_ring, 1)
    go(dn_job)
    link = Link(sum_sems, rows_all, ["pair", "ring"])
    for t in range(N_TP):
        if t % 4 == 0:
            go(hid_ring, 1)
        weights = wd[2 * t : 2 * t + 2, mine].reshape(W, 256)
        block = lax.dot_general(shared[...], weights, dims(1, 1), preferred_element_type=f32)
        part[t] = block.astype(bf16)
        if t % 2:
            i = t // 2
            link.send(part.at[2 * i + 1 - core], pair.at[i], "pair", other, "pair")
    link.arrive_all("pair", NZ * TOK_DEV)

    way = {1: 0, -1: 1}

    def term(m, rows):
        at = around(z, m, NZ)
        return part[at * 2 + core, rows].astype(f32) + pair[at, rows].astype(f32)

    def sum_round(k):
        for h, rows in enumerate(cuts):
            for d in (1, -1):
                most = reach(d, h)
                if k > most:
                    continue
                total = term(d * (most + 1 - k), rows)
                if k > 1:
                    link.arrive(got.at[way[d], k - 1, rows], (d, k - 1, h), other, "ring")
                    total = total + got[way[d], k - 1, rows].astype(f32)
                made[way[d], k, rows] = total.astype(bf16)
                src, dst = made.at[way[d], k, rows], got.at[way[d], k, rows]
                beside = z_device(around(z, d, NZ), core)
                link.send(src, dst, (d, k, h), beside, "ring")


    @on_core(1)
    def _():
        pl.semaphore_signal(turn_sem, inc=1, device_id=other, device_id_type=MESH)

    @on_core(0)
    def _():
        pl.semaphore_wait(turn_sem, 1)

    sum_round(1)
    go(hid_ring, 4)
    go(hid_ring)

    give = []
    for e in range(EXP_DEV):
        full = hid_all[e * 8 : (e + 1) * 8].reshape(F, CAP)
        outputs = jnp.dot(ed_t[e], full, preferred_element_type=f32)
        weighted = (outputs * gates_ref[e : e + 1, :]).astype(bf16)
        slots = lax.dot_general(spread[e], weighted, dims(1, 1), preferred_element_type=f32)
        back[e] = slots.astype(bf16).reshape(N_EP, ROOM, W)
        give.append(
            Exchange(
                lambda p, e=e: back.at[e, p, first],
                lambda p, e=e: returned.at[p, e, first],
                back.at[e, some, first],
                returned.at[some, e, first],
                (back_a, back_b)[e],
            )
        )
        give[e].start()

    for k in range(2, 5):
        sum_round(k)
    for h, rows in enumerate(cuts):
        total = term(0, rows)
        for d in (1, -1):
            most = reach(d, h)
            link.arrive(got.at[way[d], most, rows], (d, most, h), other, "ring")
            total = total + got[way[d], most, rows].astype(f32)
        mixed_ref[rows, :] = total
    for e in range(EXP_DEV):
        give[e].arrive()
    mixed_ref[...] += jnp.dot(
        one_t[...], returned[...].reshape(N_EP * 2 * ROOM, W), preferred_element_type=f32
    )
    for one in (ask, *dispatch, *give):
        one.finish()
    for one in (tok_link, *x_links, gu_link, dn_link, hid_link, link):
        one.finish()


def owner_of(ids):
    return ((ids >> 7) * 171) >> 9


def on_device(
    tokens,
    norm_gain,
    shared_gate,
    shared_up,
    shared_down,
    expert_gate,
    expert_up,
    expert_down,
    chosen,
    gates,
):
    vmem = pl.BlockSpec(memory_space=pltpu.VMEM)
    hbm = pl.BlockSpec(memory_space=pltpu.HBM)
    pool = lambda *shape, dtype=bf16: pltpu.VMEM(shape, dtype)
    dma = lambda n: pltpu.SemaphoreType.DMA((n,))
    return pl.pallas_call(
        layer_kernel,
        name="layer",
        out_shape=jax.ShapeDtypeStruct((TOK_DEV, W), f32),
        in_specs=[hbm] * 10,
        out_specs=vmem,
        scratch_shapes=[
            pool(EXP_DEV, CAP, dtype=i32),
            pool(64, F_DEV),
            pool(64, F_DEV),
            pool(64, F_DEV),
            pool(TOK_DEV, W),
            pool(1, D, dtype=f32),
            pool(EXP_DEV, CAP, dtype=f32),
            pool(N_EP, 1, W, dtype=i32),
            pool(64, 384),
            pool(64, 256),
            pool(EXP_DEV, NY, W, dtype=i32),
            pool(N_EP, 1, W, dtype=i32),
            pool(TOK_DEV, N_EP * 2 * ROOM),
            pool(EXP_DEV, CAP, N_EP * ROOM),
            pool(EXP_DEV, N_EP * ROOM, CAP),
            pool(N_EP, EXP_DEV, ROOM, W),
            pool(EXP_DEV, N_EP, ROOM, W),
            pool(N_TP, TOK_DEV, W),
            pool(EXP_DEV, CAP, W),
            pool(N_TP * EXP_DEV * CAP, W),
            pool(N_EP, 2, 64, 384),
            pool(N_EP, 2, 64, 256),
            pool(F_DEV, CAP),
            pool(N_TP, F_DEV, CAP),
            pool(EXP_DEV, N_EP, ROOM, W),
            pool(N_EP, EXP_DEV, ROOM, W),
            pool(N_TP, TOK_DEV, W),
            pool(NZ, TOK_DEV, W),
            pool(2, 5, TOK_DEV, W),
            pool(2, 5, TOK_DEV, W),
            pool(F_DEV, D),
            pool(F_DEV, D),
            pool(EXP_DEV, F, W),
            pool(EXP_DEV, W, F),
            pool(TOK_DEV, D),
            pool(CAP, D),
            pool(TOK_DEV, 256),
            dma(10),
            *[dma(2)] * 5,
            pltpu.SemaphoreType.REGULAR,
            dma(20),
            *[dma(34)] * 2,
            *[dma(37)] * 2,
            dma(34),
            dma(18),
        ],
        compiler_params=pltpu.CompilerParams(
            collective_id=0, has_side_effects=True, vmem_limit_bytes=56 * 1024 * 1024
        ),
    )(
        chosen,
        shared_gate,
        shared_up,
        shared_down.T,
        tokens,
        norm_gain.reshape(1, D),
        gates,
        expert_gate.reshape(F_DEV, D),
        expert_up.reshape(F_DEV, D),
        expert_down,
    ).astype(bf16)


def solution(mesh):
    return jax.shard_map(
        on_device,
        mesh=mesh,
        in_specs=(
            P("ep", "tp"),
            P(),
            P("ep", "tp"),
            P("ep", "tp"),
            P("tp", "ep"),
            P("tp", "ep", None, None),
            P("tp", "ep", None, None),
            P("ep", None, "tp"),
            P("ep", None),
            P("ep", None),
        ),
        out_specs=P("ep", "tp"),
        check_vma=False,
    )
```

```python
import jax
import jax.numpy as jnp
from jax import lax
from jax.experimental import pallas as pl
from jax.experimental.pallas import tpu as pltpu
from jax.sharding import PartitionSpec as P

MESH = pl.DeviceIdType.MESH
EXP_DEV = 2
TOK_DEV = 384
CAP = 384
NZ, NY, NX = 8, 8, 4
N_TP, N_EP = 16, 32
SLOT, ROOM = 24, 32
F_DEV, F = 176, 1408
D, W = 2048, 128
norm_eps = 1e-06
bf16, f32, i32 = jnp.bfloat16, jnp.float32, jnp.int32


def rows_of(ref):
    count = ref.dtype.itemsize
    for n in ref.shape:
        count *= n
    return count // (2 * W)


class Link:
    def __init__(self, sems, gauge, groups):
        self.sems, self.gauge, self.groups = sems, gauge, groups
        self.keys, self.sent = {}, {}

    def _copy(self, src, dst, key, device, group):
        sent = self.groups.index(group) if group in self.groups else self._at(("sent", key))
        return pltpu.make_async_remote_copy(
            src_ref=src,
            dst_ref=dst,
            send_sem=self.sems.at[sent],
            recv_sem=self.sems.at[self._at(key)],
            device_id=device,
            device_id_type=MESH,
        )

    def _at(self, key):
        if key in self.groups:
            return len(self.groups) + self.groups.index(key)
        return 2 * len(self.groups) + self.keys.setdefault(key, len(self.keys))

    def _all(self, index, rows):
        part = self.gauge.at[pl.ds(0, rows)]
        pltpu.make_async_copy(part, part, self.sems.at[index]).wait()

    def send(self, src, dst, key, device, group, core=None, wanted=None):
        self._copy(src, dst, key, device, group).start()
        at = self.groups.index(group) if group in self.groups else self._at(("sent", key))
        self.sent.setdefault((at, core), [wanted, 0])[1] += rows_of(src)

    def arrive(self, dst, key, device, group):
        self._copy(dst, dst, key, device, group).wait_recv()

    def arrive_all(self, key, rows):
        self._all(self._at(key), rows)

    def finish(self):
        for (at, core), (wanted, rows) in self.sent.items():
            here = True if core is None else lax.rem(lax.axis_index("tp"), 2) == core
            if wanted is not None:
                here = jnp.logical_and(here, wanted())
            when(here)(lambda at=at, rows=rows: self._all(at, rows))


def when(condition):
    return (lambda f: f()) if condition is True else pl.when(condition)


def on_core(core):
    return pl.when(lax.rem(lax.axis_index("tp"), 2) == core)


def places():
    tp, ep = lax.axis_index("tp"), lax.axis_index("ep")
    return tp // 2, lax.rem(tp, 2), ep // NX, lax.rem(ep, NX)


def around(position, step, count):
    return lax.rem(position + step + count, count)


def z_device(z, core):
    return {"tp": z * 2 + core}


OFFSETS = sorted(
    [(a, b) for a in range(-3, 5) for b in range(-1, 3) if (a, b) != (0, 0)],
    key=lambda o: (o[1] % 4, -abs(o[0]), o[0]),
)


def greet():
    barrier = pltpu.get_barrier_semaphore()
    z, core, y, x = places()
    devices = [{"ep": around(y, a, NY) * NX + around(x, b, NX)} for a, b in OFFSETS]
    devices += [z_device(around(z, 1, NZ), core), z_device(around(z, -1, NZ), core)]
    devices += [z_device(z, 1 - core)]
    for device in devices:
        pl.semaphore_signal(barrier, inc=1, device_id=device, device_id_type=MESH)
    return len(devices)


class Exchange:
    def __init__(self, src, dst, src_all, dst_all, sems):
        self.src, self.dst, self.src_all, self.dst_all, self.sems = src, dst, src_all, dst_all, sems

    def start(self):
        _, _, y, x = places()
        own = y * NX + x
        for a, b in OFFSETS:
            peer = around(y, a, NY) * NX + around(x, b, NX)
            pltpu.make_async_remote_copy(
                src_ref=self.src(peer),
                dst_ref=self.dst(own),
                send_sem=self.sems.at[0],
                recv_sem=self.sems.at[1],
                device_id={"ep": peer},
                device_id_type=MESH,
            ).start()
        self.dst(own)[...] = self.src(own)[...]

    def arrive(self):
        part = self.dst_all
        pltpu.make_async_copy(part, part, self.sems.at[1]).wait()

    def finish(self):
        part = self.src_all
        pltpu.make_async_copy(part, part, self.sems.at[0]).wait()


def reach(direction, flipped):
    return 4 if (direction > 0) != bool(flipped) else 3


def ring_gather(pieces, link, taker=None):
    def place():
        return lax.axis_index("tp") // 2

    def beside(d):
        return z_device(around(place(), d, NZ), 1)

    def mate(core):
        return z_device(place(), core)

    def takes():
        return True if taker is None else place() // (NZ // EXP_DEV) == taker

    def goes(d, k, flip, back):
        if taker is None:
            return True
        half = NZ // EXP_DEV
        v = lax.rem(place() - d * back - half * taker + 2 * NZ, NZ)
        if d < 0:
            v = lax.rem(half - 1 - v + NZ, NZ)
        last = half - 1 if reach(d, flip) == half else half
        return jnp.logical_or(v < half - k, v > last)

    def ring(src, at, d, k, h, c, flip, back):
        key, group = (d, k, h, c), "ring" if taker is None else None
        wanted = None if taker is None else lambda: goes(d, k, flip, back)
        link.send(src, at, key, beside(d), group, 1, wanted)

    def hand(src, dst):
        link.send(src, dst, "hand", mate(0), "hand", 1, None if taker is None else takes)
        handed.append(rows_of(src))

    handed = []
    numbered = list(enumerate(pieces))
    order = [(c, h, (flip + c) % 2, at) for c in (1, 0) for h, (flip, src, at) in numbered]
    whole = sum(rows_of(src) for flip, src, at in pieces)

    @on_core(1)
    def _():
        for h, (flip, src, at) in numbered:
            for d in (1, -1):

                @when(goes(d, 1, (flip + 1) % 2, 0))
                def _(d=d, h=h, flip=flip, src=src, at=at):
                    ring(src, at(place() * 2 + 1), d, 1, h, 1, (flip + 1) % 2, 0)

        for flip, src, at in pieces:
            when(takes())(lambda src=src, at=at: hand(src, at(place() * 2 + 1)))

    @on_core(0)
    def _():
        for flip, src, at in pieces:
            link.send(src, at(place() * 2), "join", mate(1), "join", 0)

    for flip, src, at in pieces:
        at(lax.axis_index("tp"))[...] = src[...]

    @on_core(1)
    def _():
        link.arrive_all("join", whole)
        for h, (flip, src, at) in numbered:
            for d in (1, -1):

                @when(goes(d, 1, flip, 0))
                def _(d=d, h=h, flip=flip, at=at):
                    ring(at(place() * 2), at(place() * 2), d, 1, h, 0, flip, 0)

    yield
    for k in range(1, 5):
        for c, h, flip, at in order:

            def step(d, k=k, c=c, h=h, flip=flip, at=at):
                block = at(around(place(), -d * k, NZ) * 2 + c)
                link.arrive(block, (d, k, h, c), mate(0), "ring" if taker is None else None)
                if k < reach(d, flip):
                    when(goes(d, k + 1, flip, k))(lambda: ring(block, block, d, k + 1, h, c, flip, k))
                when(takes())(lambda: hand(block, block))

            @on_core(1)
            def _(k=k, flip=flip, step=step):
                for d in (1, -1):
                    if k <= reach(d, flip):
                        when(goes(d, k, flip, k))(lambda d=d: step(d))

            yield

    @on_core(0)
    def _():
        when(takes())(lambda: link.arrive_all("hand", sum(handed)))

    yield


def plane_gather(src, dst, link, y_first):
    na, nb = (NY, NX) if y_first else (NX, NY)

    def at(da=0, db=0):
        _, _, y, x = places()
        if y_first:
            return around(y, da, NY) * NX + around(x, db, NX)
        return around(y, db, NY) * NX + around(x, da, NX)

    def mate(core):
        return z_device(places()[0], core)

    def ring(block, key, da, db):
        link.send(block, block, key, {"ep": at(da, db)}, "ring", 0)

    def hand(block):
        link.send(block.at[1], block.at[1], "hand", mate(1), "hand", 0)
        handed.append(rows_of(src))

    handed = []

    @on_core(1)
    def _():
        link.send(src, dst.at[at(), 1], "join", mate(0), "join", 1)

    dst[at(), lax.rem(lax.axis_index("tp"), 2)] = src[...]
    yield

    @on_core(0)
    def _():
        link.arrive_all("join", rows_of(src))
        block = dst.at[at()]
        for d in (1, -1):
            ring(block, ("a", d, 1), d, 0)
        for s in (1, -1):
            ring(block, ("b", s, 1, 0), 0, s)

    yield
    def most(d, n, length):
        return length // 2 if (d > 0) == (n % 2 == 0) else length // 2 - 1

    tags = [(0, 0)] + [(d, k) for k in range(1, na // 2 + 1) for d in (1, -1) if k <= most(d, 0, na)]
    for wave in range(1, na // 2 + nb // 2 + 1):

        @on_core(0)
        def _(wave=wave):
            for n, (d, k) in enumerate(tags):
                if k == wave:
                    block = dst.at[at(-d * k, 0)]
                    link.arrive(block, ("a", d, k), {"ep": at()}, "ring")
                    if k < most(d, 0, na):
                        ring(block, ("a", d, k + 1), d, 0)
                    for s in (1, -1):
                        ring(block, ("b", s, 1, n), 0, s)
                    hand(block)
            for n, (d, k) in enumerate(tags):
                j = wave - k
                for s in (1, -1):
                    if not 1 <= j <= most(s, n, nb):
                        continue
                    block = dst.at[at(-d * k, -s * j)]
                    link.arrive(block, ("b", s, j, n), {"ep": at()}, "ring")
                    if j < most(s, n, nb):
                        ring(block, ("b", s, j + 1, n), 0, s)
                    hand(block)

        yield

    @on_core(1)
    def _():
        link.arrive_all("hand", sum(handed))

    yield


def go(job, steps=1000):
    for _ in range(steps):
        if next(job, "end") == "end":
            return


def one_hot(condition):
    return jnp.where(condition, 1.0, 0.0).astype(bf16)


def silu(v):
    return v / (1.0 + jnp.exp(-v))


def dims(a, b):
    return (((a,), (b,)), ((), ()))


def normalise(blocks, gain_ref, out_ref):
    for r in range(0, TOK_DEV, W):
        rows = pl.ds(r, W)
        squares = jnp.zeros((W, W), f32)
        for t in range(N_TP):
            wide = blocks(t)[rows, :].astype(f32)
            squares = squares + wide * wide
        inv = lax.rsqrt(jnp.sum(squares, axis=1, keepdims=True) * (1.0 / D) + norm_eps)
        for t in range(N_TP):
            lanes = slice(t * W, (t + 1) * W)
            wide = blocks(t)[rows, :].astype(f32)
            out_ref[rows, lanes] = (wide * inv * gain_ref[:, lanes]).astype(bf16)


def layer_kernel(
    chosen_hbm, sg_hbm, su_hbm, sd_hbm, tok_hbm, gain_hbm, gates_hbm, eg_hbm, eu_hbm, ed_hbm,
    mixed_ref,
    chosen_ref, sg_ref, su_ref, sd_ref, tok_ref, gain_ref, gates_ref,
    req_ref, gu_ref, dn_ref, wanted, asked, one_t, join, spread, out, came, tok_all, own, rows_all, wg, wd, hid, hid_all, back, returned,
    part, pair, got, made, eg, eu, ed, ed_t, normed, taken, shared, slot_columns,
    load_sem, ask_sem, go_a, go_b, back_a, back_b,
    turn_sem, tok_sems, xa_sems, xb_sems, gu_sems, dn_sems, hid_sems, sum_sems,
):
    z, core, _, _ = places()
    other = z_device(z, 1 - core)
    loads = [
        pltpu.make_async_copy(s, d, load_sem.at[i])
        for i, (s, d) in enumerate(
            (
                (chosen_hbm, chosen_ref),
                (sg_hbm, sg_ref),
                (su_hbm, su_ref),
                (sd_hbm, sd_ref),
                (tok_hbm, tok_ref),
                (gain_hbm, gain_ref),
                (gates_hbm, gates_ref),
                (eg_hbm, eg),
                (eu_hbm, eu),
                (ed_hbm, ed),
            )
        )
    ]
    for load in loads:
        load.start()
    count = greet()
    loads[0].wait()
    slot_rows = []
    lane = lax.broadcasted_iota(i32, (CAP, W), 1)
    for e in range(EXP_DEV):
        ids = chosen_ref[e : e + 1, :]
        sources = owner_of(ids)
        ids_down = jnp.broadcast_to(ids, (W, CAP)).T
        sources_down = owner_of(ids_down)
        before = jnp.sum(
            jnp.where(jnp.concatenate([sources_down] * 3, axis=1) < sources, 1, 0), axis=0, keepdims=True
        )
        slots = sources * ROOM + lax.broadcasted_iota(i32, (1, CAP), 1) - before
        slot_rows.append(slots)
        slots_down = jnp.broadcast_to(slots, (W, CAP)).T
        slot_columns[e] = slots_down
        local = ids_down - sources_down * TOK_DEV
        for b in range(N_EP * ROOM // W):
            match = slots_down == lane + b * W
            wanted[e, b : b + 1] = jnp.max(jnp.where(match, local, -1), axis=0, keepdims=True)
    side = lax.rem(lax.axis_index("ep"), 2)
    lane = lax.broadcasted_iota(i32, (NY, W), 1)
    for i in range(NX):
        a, b = (pltpu.roll(wanted[e], (e - i) % NX * ROOM, 1) for e in range(EXP_DEV))
        both = jnp.where(lane < ROOM, a, jnp.where(lane < 2 * ROOM, b, -1))
        both = jnp.where(side == 0, both, pltpu.roll(both, W // 2, 1))
        for j in range(NY):
            req_ref[j * NX + i] = both[j : j + 1]
    came[...] = jnp.zeros_like(came)
    loads[4].wait()
    pl.semaphore_wait(pltpu.get_barrier_semaphore(), count)

    half = TOK_DEV // 2
    cuts = [pl.ds(0, half), pl.ds(half, half)]
    first = pl.ds(0, SLOT)
    some = pl.ds(0, N_EP - 1)

    half = TOK_DEV // 2
    cuts = [pl.ds(0, half), pl.ds(half, half)]
    first = pl.ds(0, SLOT)
    some = pl.ds(0, N_EP - 1)
    ask = Exchange(
        lambda p: req_ref.at[p], lambda p: asked.at[p], req_ref.at[some], asked.at[some], ask_sem
    )
    ask.start()
    kinds = ["ring", "hand", "join"]
    tok_link = Link(tok_sems, rows_all, kinds)
    tok_ring = ring_gather(
        [(0, tok_ref, lambda t: tok_all.at[t])], tok_link
    )
    go(tok_ring, 1)
    for load in loads[1:4]:
        load.wait()
    returned[...] = jnp.zeros_like(returned)
    gu_ref[:, :W] = sg_ref[:, :W]
    gu_ref[:, W : 2 * W] = su_ref[:, :W]
    gu_ref[:, 2 * W :] = jnp.concatenate(
        [sg_ref[:, W:], su_ref[:, W:], jnp.zeros((64, 32), bf16)], axis=1
    )
    dn_ref[...] = jnp.concatenate([sd_ref[...], jnp.zeros((64, 80), bf16)], axis=1)
    gu_link, dn_link = Link(gu_sems, rows_all, kinds), Link(dn_sems, rows_all, kinds)
    gu_job = plane_gather(gu_ref, wg, gu_link, True)
    dn_job = plane_gather(dn_ref, wd, dn_link, False)
    go(gu_job, 1)
    go(dn_job, 1)
    for e in range(EXP_DEV):
        at = lax.broadcasted_iota(i32, (N_EP * ROOM, CAP), 0)
        spread[e] = one_hot(at == slot_rows[e])
        lane = lax.broadcasted_iota(i32, (CAP, W), 1)
        for b in range(N_EP * ROOM // W):
            join[e, :, b * W : (b + 1) * W] = one_hot(slot_columns[e] == lane + b * W)
    go(gu_job, 1)
    go(dn_job, 1)
    go(tok_ring, 2)

    ask.arrive()
    token = lax.broadcasted_iota(i32, (TOK_DEV, W), 0)
    for i in range(N_EP // 2):
        ids = jnp.maximum(asked[2 * i], asked[2 * i + 1])
        one_t[:, i * W : (i + 1) * W] = one_hot(token == ids)
    for i in range(4):
        lanes = slice(i * 512, (i + 1) * 512)
        picked = lax.dot_general(
            one_t[:, lanes], tok_ref[...], dims(0, 0), preferred_element_type=f32
        )
        out[i * 8 : (i + 1) * 8] = picked.astype(bf16).reshape(8, EXP_DEV, ROOM, W)
    dispatch = [
        Exchange(
            lambda p, e=e: out.at[p, e, first],
            lambda p, e=e: came.at[e, p, first],
            out.at[some, e, first],
            came.at[e, some, first],
            sem,
        )
        for e, sem in enumerate((go_a, go_b))
    ]
    for e in range(EXP_DEV):
        dispatch[e].start()
    for load in loads[5:]:
        load.wait()
    for e in range(EXP_DEV):
        ed_t[e] = ed[e].T
    go(tok_ring, 2)
    go(tok_ring, 2)

    x_links = [Link(xa_sems, rows_all, kinds), Link(xb_sems, rows_all, kinds)]
    x_rings = []

    def taken_rows(t, e):
        return pl.ds(pl.multiple_of((t * EXP_DEV + e) * CAP, CAP), CAP)

    for e in range(EXP_DEV):
        dispatch[e].arrive()
        own[e] = jnp.dot(
            join[e], came[e].reshape(N_EP * ROOM, W), preferred_element_type=f32
        ).astype(bf16)
        x_rings.append(
            ring_gather(
                [(e, own.at[e], lambda t, e=e: rows_all.at[taken_rows(t, e)])],
                x_links[e],
                e,
            )
        )
        go(x_rings[e], 1)
        if e == 0:
            go(tok_ring, 2)
            go(gu_job, 1)
            go(dn_job, 1)
    for wave in range(3):
        go(gu_job, 1)
        go(dn_job, 1)
    for k in range(4):
        for e in range(EXP_DEV):
            go(x_rings[e], 2)
    for e in range(EXP_DEV):
        go(x_rings[e], 1)

    expert = z // (NZ // EXP_DEV)
    normalise(lambda t: rows_all.at[taken_rows(t, expert)], gain_ref, taken)
    gate_values = lax.dot_general(eg[...], taken[...], dims(1, 1), preferred_element_type=f32)
    up_values = lax.dot_general(eu[...], taken[...], dims(1, 1), preferred_element_type=f32)
    hid[...] = (silu(gate_values) * up_values).astype(bf16)
    hid_link = Link(hid_sems, rows_all, kinds)
    hid_ring = ring_gather(
        [
            (h, hid.at[c], lambda t, c=c: hid_all.at[t, c])
            for h, c in enumerate((pl.ds(0, 96), pl.ds(96, 80)))
        ],
        hid_link,
    )
    go(hid_ring, 1)

    go(tok_ring)
    normalise(lambda t: tok_all.at[t], gain_ref, normed)
    for wave in range(2):
        go(gu_job, 1)
        go(dn_job, 1)
    go(hid_ring, 4)
    go(gu_job)
    go(hid_ring, 1)
    mine = pl.ds(core, 1)
    weights = wg[:, mine].reshape(D, 384)
    for i in range(3):
        block = pl.ds(i * W, W)
        sums = jnp.dot(normed[block, :], weights, preferred_element_type=f32)
        low = silu(sums[:, :W]) * sums[:, W : 2 * W]
        high = silu(sums[:, 256:304]) * sums[:, 304:352]
        shared[block, :] = jnp.concatenate([low, high, jnp.zeros((W, 80), f32)], axis=1).astype(bf16)
        go(hid_ring, 1)
    go(dn_job)
    link = Link(sum_sems, rows_all, ["pair", "ring"])
    for t in range(N_TP):
        if t % 4 == 0:
            go(hid_ring, 1)
        weights = wd[2 * t : 2 * t + 2, mine].reshape(W, 256)
        block = lax.dot_general(shared[...], weights, dims(1, 1), preferred_element_type=f32)
        part[t] = block.astype(bf16)
        if t % 2:
            i = t // 2
            link.send(part.at[2 * i + 1 - core], pair.at[i], "pair", other, "pair")
    link.arrive_all("pair", NZ * TOK_DEV)

    way = {1: 0, -1: 1}

    def term(m, rows):
        at = around(z, m, NZ)
        return part[at * 2 + core, rows].astype(f32) + pair[at, rows].astype(f32)

    def sum_round(k):
        for h, rows in enumerate(cuts):
            for d in (1, -1):
                most = reach(d, h)
                if k > most:
                    continue
                total = term(d * (most + 1 - k), rows)
                if k > 1:
                    link.arrive(got.at[way[d], k - 1, rows], (d, k - 1, h), other, "ring")
                    total = total + got[way[d], k - 1, rows].astype(f32)
                made[way[d], k, rows] = total.astype(bf16)
                src, dst = made.at[way[d], k, rows], got.at[way[d], k, rows]
                beside = z_device(around(z, d, NZ), core)
                link.send(src, dst, (d, k, h), beside, "ring")


    @on_core(1)
    def _():
        pl.semaphore_signal(turn_sem, inc=1, device_id=other, device_id_type=MESH)

    @on_core(0)
    def _():
        pl.semaphore_wait(turn_sem, 1)

    sum_round(1)
    go(hid_ring, 4)
    go(hid_ring)

    give = []
    for e in range(EXP_DEV):
        full = hid_all[e * 8 : (e + 1) * 8].reshape(F, CAP)
        outputs = jnp.dot(ed_t[e], full, preferred_element_type=f32)
        weighted = (outputs * gates_ref[e : e + 1, :]).astype(bf16)
        slots = lax.dot_general(spread[e], weighted, dims(1, 1), preferred_element_type=f32)
        back[e] = slots.astype(bf16).reshape(N_EP, ROOM, W)
        give.append(
            Exchange(
                lambda p, e=e: back.at[e, p, first],
                lambda p, e=e: returned.at[p, e, first],
                back.at[e, some, first],
                returned.at[some, e, first],
                (back_a, back_b)[e],
            )
        )
        give[e].start()

    for k in range(2, 5):
        sum_round(k)
    for h, rows in enumerate(cuts):
        total = term(0, rows)
        for d in (1, -1):
            most = reach(d, h)
            link.arrive(got.at[way[d], most, rows], (d, most, h), other, "ring")
            total = total + got[way[d], most, rows].astype(f32)
        mixed_ref[rows, :] = total
    for e in range(EXP_DEV):
        give[e].arrive()
    mixed_ref[...] += jnp.dot(
        one_t[...], returned[...].reshape(N_EP * 2 * ROOM, W), preferred_element_type=f32
    )
    for one in (ask, *dispatch, *give):
        one.finish()
    for one in (tok_link, *x_links, gu_link, dn_link, hid_link, link):
        one.finish()


def owner_of(ids):
    return ((ids >> 7) * 171) >> 9


def on_device(
    tokens,
    norm_gain,
    shared_gate,
    shared_up,
    shared_down,
    expert_gate,
    expert_up,
    expert_down,
    chosen,
    gates,
):
    vmem = pl.BlockSpec(memory_space=pltpu.VMEM)
    hbm = pl.BlockSpec(memory_space=pltpu.HBM)
    pool = lambda *shape, dtype=bf16: pltpu.VMEM(shape, dtype)
    dma = lambda n: pltpu.SemaphoreType.DMA((n,))
    return pl.pallas_call(
        layer_kernel,
        name="layer",
        out_shape=jax.ShapeDtypeStruct((TOK_DEV, W), f32),
        in_specs=[hbm] * 10,
        out_specs=vmem,
        scratch_shapes=[
            pool(EXP_DEV, CAP, dtype=i32),
            pool(64, F_DEV),
            pool(64, F_DEV),
            pool(64, F_DEV),
            pool(TOK_DEV, W),
            pool(1, D, dtype=f32),
            pool(EXP_DEV, CAP, dtype=f32),
            pool(N_EP, 1, W, dtype=i32),
            pool(64, 384),
            pool(64, 256),
            pool(EXP_DEV, NY, W, dtype=i32),
            pool(N_EP, 1, W, dtype=i32),
            pool(TOK_DEV, N_EP * 2 * ROOM),
            pool(EXP_DEV, CAP, N_EP * ROOM),
            pool(EXP_DEV, N_EP * ROOM, CAP),
            pool(N_EP, EXP_DEV, ROOM, W),
            pool(EXP_DEV, N_EP, ROOM, W),
            pool(N_TP, TOK_DEV, W),
            pool(EXP_DEV, CAP, W),
            pool(N_TP * EXP_DEV * CAP, W),
            pool(N_EP, 2, 64, 384),
            pool(N_EP, 2, 64, 256),
            pool(F_DEV, CAP),
            pool(N_TP, F_DEV, CAP),
            pool(EXP_DEV, N_EP, ROOM, W),
            pool(N_EP, EXP_DEV, ROOM, W),
            pool(N_TP, TOK_DEV, W),
            pool(NZ, TOK_DEV, W),
            pool(2, 5, TOK_DEV, W),
            pool(2, 5, TOK_DEV, W),
            pool(F_DEV, D),
            pool(F_DEV, D),
            pool(EXP_DEV, F, W),
            pool(EXP_DEV, W, F),
            pool(TOK_DEV, D),
            pool(CAP, D),
            pool(TOK_DEV, 256),
            pool(EXP_DEV, CAP, W, dtype=i32),
            dma(10),
            *[dma(2)] * 5,
            pltpu.SemaphoreType.REGULAR,
            dma(20),
            *[dma(34)] * 2,
            *[dma(37)] * 2,
            dma(34),
            dma(18),
        ],
        compiler_params=pltpu.CompilerParams(
            collective_id=0, has_side_effects=True, vmem_limit_bytes=56 * 1024 * 1024
        ),
    )(
        chosen,
        shared_gate,
        shared_up,
        shared_down.T,
        tokens,
        norm_gain.reshape(1, D),
        gates,
        expert_gate.reshape(F_DEV, D),
        expert_up.reshape(F_DEV, D),
        expert_down,
    ).astype(bf16)


def solution(mesh):
    return jax.shard_map(
        on_device,
        mesh=mesh,
        in_specs=(
            P("ep", "tp"),
            P(),
            P("ep", "tp"),
            P("ep", "tp"),
            P("tp", "ep"),
            P("tp", "ep", None, None),
            P("tp", "ep", None, None),
            P("ep", None, "tp"),
            P("ep", None),
            P("ep", None),
        ),
        out_specs=P("ep", "tp"),
        check_vma=False,
    )
```
